128 devices in a mesh: fsdp: 128 (over x, z, y, core).
Axes of the slice: x: 4, y: 4, z: 4, core: 2. Of those that a mesh axis runs over, the one named last changes fastest.
Arguments:
- statistics: float32 [128, 1024, 1024], P(None, 'fsdp'), may hold values from -60 to 200, as said below
- gradient: bfloat16 [128, 1024, 1024], P(None, 'fsdp'), may hold values from -24 to 24
- block_slot: int32 [128], replicated, may hold values from 0 to 127, each once
Outputs:
- new_statistics: float32 [128, 1024, 1024], P(None, 'fsdp')
- slot_roots: float32 [128, 1024, 1024], P('fsdp')
- update: float32 [128, 1024, 1024], P(None, 'fsdp')
The draws below stay inside these ranges and needn't reach their ends.
Inputs may be any that keep to these rules, and one draw needn't show every extreme that they name: block_slot is a permutation of 0 to 127. Every block of statistics is symmetric with all eigenvalues at least 10.
All inputs are finite; a program needn't handle non-finite values.
Results may differ from the reference program's by a relative error of at most 0.0003.
Values may be sent and summed in bfloat16 or wider, within the bound.
A program may use at most 128 MiB of HBM per device.

```python
import jax
import jax.numpy as jnp
from jax import lax

B = 1024
ITERS = 4
NBLK = 128


def draw_statistics(key, part):
    low_key = jax.random.fold_in(key, 11)
    diag_key = jax.random.fold_in(key, 12)
    factors = jax.random.normal(low_key, (NBLK, B, 64), jnp.float32)
    gram = jnp.einsum('kir,kjr->kij', factors, factors) / 64.0
    gram = 0.5 * (gram + jnp.swapaxes(gram, 1, 2))
    floor = jax.random.uniform(diag_key, (NBLK, B), jnp.float32, 0.5, 1.5)
    return 40.0 * gram + 20.0 * floor[:, :, None] * jnp.eye(B, dtype=jnp.float32)[None, :, :]


def strengthened(entries, stream_key, source, target, blocks, factor):
    def block_of(position):
        return (jnp.arange(entries.shape[position]) // (entries.shape[position] // blocks)).reshape((-1,) + (1,) * (entries.ndim - 1 - position))

    one_side = jax.random.permutation(stream_key, blocks)[block_of(target)]
    other_side = (block_of(target) + blocks // 2) % blocks
    return jnp.where((block_of(source) == one_side) | (block_of(source) == other_side), factor * entries, entries)


def block_scale(rng, shape, shards, least, top_value):
    gain = 1.0
    for axis_at, shards_of in shards:
        draws = jax.random.uniform(jax.random.fold_in(jax.random.fold_in(rng, 6), axis_at), (shards_of,), jnp.float32, least / len(shards), top_value / len(shards))
        gain = gain * jnp.repeat(jnp.exp(draws), shape[axis_at] // shards_of).reshape((-1,) + (1,) * (len(shape) - 1 - axis_at))
    return gain


def heavy_noise(own_key, dims, scale, reach, split, heavy, kind=jnp.bfloat16):
    drawn = scale * jax.random.normal(own_key, dims, jnp.float32)
    if split:
        drawn = drawn * block_scale(own_key, dims, split, -0.22, 0.18)
    return jnp.clip(strengthened(drawn, jax.random.fold_in(own_key, 3), *heavy), -reach, reach).astype(kind)


def setup_inputs(seed: int = 0) -> dict:
    key_list = jax.random.split(jax.random.key(seed), 4)
    return {
        "statistics": draw_statistics(jax.random.fold_in(key_list[3], 71), 0),
        "gradient": heavy_noise(key_list[1], (NBLK, B, B), 1.0, 24.0, ((1, 128),), (1, 0, 128, 5.5)),
        "block_slot": jax.random.permutation(key_list[2], NBLK).astype(jnp.int32),
    }


stat_decay = 0.95
ridge_scale = 0.001

def inverse_root(matrix):
    block_width = matrix.shape[0]
    identity = jnp.eye(block_width, dtype=jnp.float32)
    frobenius = jnp.sqrt(jnp.sum(matrix * matrix))
    shrink = 2.5 / frobenius
    current = shrink * matrix
    result_root = jnp.sqrt(jnp.sqrt(shrink)) * identity
    for iteration in range(ITERS):
        factor = (5.0 * identity - current) * 0.25
        result_root = jnp.dot(result_root, factor, precision=lax.Precision.HIGHEST)
        square = jnp.dot(factor, factor, precision=lax.Precision.HIGHEST)
        fourth = jnp.dot(square, square, precision=lax.Precision.HIGHEST)
        current = jnp.dot(fourth, current, precision=lax.Precision.HIGHEST)
    return result_root

def refresh_block(stat_block, grad_block):
    block_width = stat_block.shape[0]
    outer = jnp.dot(grad_block, grad_block.T, preferred_element_type=jnp.float32)
    renewed = stat_decay * stat_block + (1.0 - stat_decay) * outer
    diag_sum = jnp.trace(renewed)
    damped = renewed + ridge_scale * (diag_sum / block_width) * jnp.eye(block_width, dtype=jnp.float32)
    root_block = inverse_root(damped)
    raw_block = jnp.dot(root_block, grad_block.astype(jnp.float32), precision=lax.Precision.HIGHEST)
    return (renewed, root_block, raw_block)

def reference(statistics, gradient, block_slot):
    renewed, roots, raw_update = lax.map(lambda operands: refresh_block(operands[0], operands[1]), (statistics, gradient))
    grad_sq = jnp.sum(jnp.square(gradient.astype(jnp.float32)))
    raw_sq = jnp.sum(raw_update * raw_update)
    graft_ratio = jnp.sqrt(grad_sq) / jnp.sqrt(raw_sq)
    block_count = block_slot.shape[0]
    placed = jnp.zeros((block_count,), jnp.int32).at[block_slot].set(jnp.arange(block_count, dtype=jnp.int32))
    return (renewed, roots[placed], graft_ratio * raw_update)
```

```python
import itertools

import jax
import jax.numpy as jnp
from jax import lax
from jax.experimental import pallas as pl
from jax.experimental.pallas import tpu as pltpu
from jax.sharding import PartitionSpec as P

N = 128
B = 1024
ROWS = 8
AXIS = "fsdp"
MESH = pl.DeviceIdType.MESH
F32 = jnp.float32
BF16 = jnp.bfloat16
I16 = jnp.int16
I32 = jnp.int32

STAT_DECAY = 0.95
RIDGE = 0.001
STAT_MAX = 200.0
TOP = 32760.0
PANEL = 256
PANELS = B // PANEL
TINY = 1e-30

CHIPS = [o for o in itertools.product(range(4), repeat=3) if any(o)]
HOPS = (0, 1, 2, 1)
FAR_FIRST = sorted(CHIPS, key=lambda o: -sum(HOPS[k] for k in o))
ROUND = [((2, 1, 3, 0)[j % 4], (5 * j + 3) % 16 // 4, (5 * j + 3) % 4) for j in range(16)]


def quarter_code(x, inverse_max):
    unit = x * inverse_max
    a = jnp.abs(unit) + TINY
    r = lax.rsqrt(a)
    s = lax.rsqrt(a * r)
    return jnp.round(unit * r * s * TOP).astype(I32).astype(I16)


def quarter_value(q, top_to_value):
    y = q.astype(I32).astype(F32)
    return (y * y) * (y * jnp.abs(y)) * top_to_value


def half_code(x, scale):
    return jnp.round(x * lax.rsqrt(jnp.abs(x) + TINY) * scale).astype(I32).astype(I16)


def half_value(q, scale):
    y = q.astype(I32).astype(F32)
    return y * jnp.abs(y) * scale


def eye_block():
    return (lax.broadcasted_iota(I32, (128, 128), 0) == lax.broadcasted_iota(I32, (128, 128), 1)).astype(F32)


def product(a, b):
    return jnp.dot(a, b, preferred_element_type=F32)


def below(p):
    return slice(PANEL * p, PANEL * (p + 1)), slice(PANEL * p, B)


def mirror(p, value, put):
    rows, cols = below(p)
    put(rows, cols, value)
    if p + 1 < PANELS:
        put(slice(PANEL * (p + 1), B), rows, value[:, PANEL:].T)


def put_bf16(ref):
    def put(rows, cols, value):
        ref[rows, cols] = value.astype(BF16)

    return put


def put_split(high, low):
    def put(rows, cols, value):
        hi = value.astype(BF16)
        high[rows, cols] = hi
        low[rows, cols] = (value - hi.astype(F32)).astype(BF16)

    return put


def exchange_kernel(
    slot_hbm, stat_hbm, grad_hbm, stat, root, outer_in, raw_in, misc_in,
    slots, placed_row, placed, gin, gsend, ssend, grecv, srecv, gm, nf, vf, nb, nl, sb, zb, vb, code, msend,
    load_p, load_g, load_s, g_out, g_in, s_out, s_in, e_out, e_in, o_out, o_in, r_out, r_in, m_out, m_in,
):
    sf = root
    me = lax.axis_index(AXIS)
    core = lax.rem(me, 2)
    sibling = me + 1 - 2 * core
    y = lax.rem(me // 2, 4)
    z = lax.rem(me // 8, 4)
    x = me // 32
    block_row = me // 16
    high = me // 64
    bit = lax.rem(me // 2, 2)
    at_x = [lax.rem(x + k, 4) * 32 for k in range(4)]
    at_z = [lax.rem(z + k, 4) * 8 for k in range(4)]
    at_y = [lax.rem(y + k, 4) * 2 for k in range(4)]

    def send(src, dst, out_sem, in_sem, target):
        pltpu.make_async_remote_copy(
            src_ref=src, dst_ref=dst, send_sem=out_sem, recv_sem=in_sem,
            device_id={AXIS: target}, device_id_type=MESH,
        ).start()

    def to_chips(cores, go):
        def step(i, carry):
            for kx, kz, ky in ROUND:
                chip = lax.rem(x + kx + i, 4) * 32 + at_z[kz] + at_y[ky]
                for c in cores:
                    if kz == 0 and ky == 0:
                        pl.when(chip + c != me)(lambda: go(chip + c))
                    else:
                        go(chip + c)
            return carry

        lax.fori_loop(0, 4, step, 0)

    barrier = pltpu.get_barrier_semaphore()
    get_p = pltpu.make_async_copy(slot_hbm, slots.at[0], load_p)
    get_g = pltpu.make_async_copy(grad_hbm, gin, load_g)
    get_s = pltpu.make_async_copy(stat_hbm, stat, load_s)
    get_p.start()
    get_g.start()
    get_s.start()

    with jax.named_scope("greet"):
        for o in FAR_FIRST:
            for c in (0, 1):
                other = at_x[o[0]] + at_z[o[1]] + at_y[o[2]] + c
                pl.semaphore_signal(barrier, inc=1, device_id={AXIS: other}, device_id_type=MESH)
        pl.semaphore_signal(barrier, inc=1, device_id={AXIS: sibling}, device_id_type=MESH)

    with jax.named_scope("placed"):
        get_p.wait()
        down = jnp.broadcast_to(slots[...], (128, 128)).T
        hit = down == lax.broadcasted_iota(I32, (128, 128), 1)
        placed_row[...] = jnp.max(
            jnp.where(hit, lax.broadcasted_iota(I32, (128, 128), 0), 0), axis=0, keepdims=True
        )
        put_p = pltpu.make_async_copy(placed_row, placed, load_p)
        put_p.start()
        get_g.wait()
        put_p.wait()

    def pack_g(s, carry):
        gsend[s] = gin[placed[0, s]]
        return carry

    with jax.named_scope("pack_g"):
        lax.fori_loop(0, N, pack_g, 0, unroll=4)
    get_s.wait()
    stat_scale = TOP / (STAT_MAX**0.5)

    def pack_s(group):
        def step(i, carry):
            s = 2 * i + group
            b = placed[0, s]
            for j in range(5):
                column = pl.multiple_of(lax.rem(block_row + j, 8) * 128, 128)
                ssend[s, :, 128 * j : 128 * (j + 1)] = half_code(stat[b, :, pl.ds(column, 128)], stat_scale)
            return carry

        with jax.named_scope("pack_s"):
            lax.fori_loop(0, N // 2, step, 0, unroll=4)

    with jax.named_scope("wait_barrier"):
        pl.semaphore_wait(barrier, N - 1)

    def send_g(target, half):
        cols = pl.ds(512 * half, 512)
        send(gsend.at[target, :, cols], grecv.at[me, :, cols], g_out, g_in, target)

    def send_s(target):
        send(ssend.at[target, :, pl.ds(0, 512)], srecv.at[me, :, pl.ds(0, 512)], s_out, s_in, target)

        @pl.when(lax.rem(target // 2, 2) == high)
        def _():
            send(ssend.at[target, :, pl.ds(512, 128)], srecv.at[me, :, pl.ds(512, 128)], e_out, e_in, target)

    for group in (0, 1):
        with jax.named_scope("send_g"):
            for half in (0, 1):
                to_chips((group,), lambda target: send_g(target, half))
        pack_s(group)
        with jax.named_scope("send_s"):
            to_chips((group,), send_s)

    grecv[me] = gsend[me]
    srecv[me] = ssend[me]

    with jax.named_scope("wait_g"):
        pltpu.make_async_copy(gsend.at[pl.ds(0, N - 1)], grecv.at[pl.ds(0, N - 1)], g_in).wait()

    def unpack_g(p, carry):
        gm[pl.ds(p * PANEL, PANEL), :] = grecv[pl.ds(p * 32, 32)].reshape(PANEL, B)
        return carry

    lane = lax.broadcasted_iota(I32, (1, 128), 1)

    def put_nf(rows, cols, value):
        nf[rows, cols] = value

    def outer_product(p):
        rows, cols = below(p)
        outer = lax.dot_general(gm[rows, :], gm[cols, :], (((1,), (1,)), ((), ())), preferred_element_type=F32)
        mirror(p, outer * (1.0 - STAT_DECAY), put_nf)

    def outer_panel(p, tops):
        rows = pl.ds(p * PANEL, PANEL)
        outer = nf[rows, :]
        top = jnp.maximum(jnp.max(jnp.abs(outer), keepdims=True), TINY)
        code[pl.ds(p * 32, 32)] = quarter_code(outer, 1.0 / top).reshape(32, ROWS, B)
        return jnp.where(lane == p, top, tops)

    with jax.named_scope("outer"):
        lax.fori_loop(0, PANELS, unpack_g, 0)
        for p in range(PANELS):
            outer_product(p)
    with jax.named_scope("outer_code"):
        outer_tops = lax.fori_loop(0, PANELS, outer_panel, jnp.zeros((1, 128), F32))

    eye = eye_block()

    def diagonal(i):
        span = pl.ds(pl.multiple_of(i * 128, 128), 128)
        return span, nf[span, span]

    def trace_step(i, total):
        return total + diagonal(i)[1] * eye

    zeros = jnp.zeros((128, 128), F32)
    grad_sq = jnp.sum(lax.fori_loop(0, 8, trace_step, zeros), keepdims=True) / (1.0 - STAT_DECAY)

    def wait_extra(count, out):
        part = pl.ds(0, count)
        pltpu.make_async_copy(
            ssend.at[part, :, pl.ds(512, 128)], srecv.at[part, :, pl.ds(512, 128)], e_out if out else e_in
        ).wait()

    def wait_extras(out):
        @pl.when(bit == high)
        def _():
            wait_extra(N // 2 - 1, out)

        @pl.when(bit != high)
        def _():
            wait_extra(N // 2, out)

    with jax.named_scope("wait_s"):
        pltpu.make_async_copy(
            ssend.at[pl.ds(0, N - 1), :, pl.ds(0, 512)], srecv.at[pl.ds(0, N - 1), :, pl.ds(0, 512)], s_in
        ).wait()
        wait_extras(False)

    stat_value = STAT_DECAY / stat_scale**2
    put_n = put_split(nb, nl)

    def add_tile(i, j, square, own):
        other = lax.rem(i + j, 8)
        tile = half_value(srecv[pl.ds(i * 16, 16), :, 128 * j : 128 * (j + 1)], stat_value).reshape(128, 128)
        rows = pl.ds(pl.multiple_of(i * 128, 128), 128)
        cols = pl.ds(pl.multiple_of(other * 128, 128), 128)
        value = nf[rows, cols] + tile
        nf[rows, cols] = value
        put_n(rows, cols, value)
        if own:
            return square + value * value
        mirrored = value.T
        nf[cols, rows] = mirrored
        put_n(cols, rows, mirrored)
        return square + 2.0 * (value * value)

    def tiles(i, square):
        for j in range(4):
            square = add_tile(i, j, square, j == 0)
        return square

    with jax.named_scope("tiles"):
        square = lax.fori_loop(0, 8, tiles, zeros)
        square = lax.fori_loop(0, 4, lambda i, acc: add_tile(i + 4 * bit, 4, acc, False), square)
        total_sq = jnp.sum(square, keepdims=True)
        trace = jnp.sum(lax.fori_loop(0, 8, trace_step, zeros), keepdims=True)
        mean = trace * (1.0 / B)
        ridge = RIDGE * mean
        total_sq = total_sq + 2.0 * ridge * trace + ridge * ridge * float(B)
        shrink = 2.5 * lax.rsqrt(total_sq)
        root_scale = lax.rsqrt(lax.rsqrt(shrink))

        def center(i, carry):
            span, value = diagonal(i)
            value = value - eye * mean
            nf[span, span] = value
            put_n(span, span, value)
            return carry

        lax.fori_loop(0, 8, center, 0)

    def send_outer():
        for half in (0, 1):
            cols = pl.ds(512 * half, 512)
            to_chips(
                (0, 1), lambda target: send(code.at[target, :, cols], outer_in.at[me, :, cols], o_out, o_in, target)
            )

    def iterate(first, k, mu, scale_y, v_unit):
        phi = (5.0 - mu) * 0.25
        phi2 = phi * phi
        phi3 = phi2 * phi
        phi4 = phi2 * phi2
        quarter_y = scale_y * 0.25
        quarter_v = v_unit * 0.25
        with jax.named_scope("square"):
            for p in range(PANELS):
                rows, cols = below(p)
                hi = nb[rows, :]
                s = product(hi, nb[:, cols]) + product(hi, nl[:, cols]) + product(nl[rows, :], nb[:, cols])
                if first:
                    s = s * (shrink * shrink)
                    vf[rows, cols] = nf[rows, cols] * (shrink * -0.25)
                    vb[1, rows, :] = hi
                else:
                    vn = product(vb[k, rows, :], nb[:, cols])
                    v = vf[rows, cols] * phi - nf[rows, cols] * quarter_y - vn * quarter_v
                    vf[rows, cols] = v
                    mirror(p, v, put_bf16(vb.at[1 - k]))
                sf[rows, cols] = s
                mirror(p, s, put_bf16(sb))
        n_n = phi4 - mu * phi3
        n_s = 0.375 * mu * phi2 - phi3
        n_t = 0.375 * phi2 - mu * phi * (1.0 / 16.0)
        z_s = mu * (1.0 / 256.0) - phi * (1.0 / 16.0)
        z_t = 1.0 / 256.0
        if first:
            n_n, n_t, z_t = n_n * shrink, n_t * shrink, z_t * shrink
        with jax.named_scope("cube"):
            for p in range(PANELS):
                rows, cols = below(p)
                t = product(sb[rows, :], nb[:, cols])
                s = sf[rows, cols]
                nf[rows, cols] = nf[rows, cols] * n_n + s * n_s + t * n_t
                mirror(p, s * z_s + t * z_t, put_bf16(zb))
        with jax.named_scope("next"):
            for p in range(PANELS):
                rows, cols = below(p)
                n = nf[rows, cols] + product(sb[rows, :], zb[:, cols])
                nf[rows, cols] = n
                mirror(p, n, put_n)
        return phi4 * mu, scale_y * phi

    one = jnp.ones((1, 1), F32)
    mu, scale_y = iterate(True, 0, shrink * mean * (1.0 + RIDGE), one, one)
    with jax.named_scope("send_outer"):
        send_outer()
        outer_in[me] = code[me]

    def later(k, carry):
        mu, scale_y, v_unit = carry
        mu, scale_y = iterate(False, lax.rem(k, 2), mu, scale_y, v_unit)
        return mu, scale_y, one

    mu, scale_y, _ = lax.fori_loop(1, 3, later, (mu, scale_y, shrink * -0.25))
    phi = (5.0 - mu) * 0.25
    diag_root = root_scale * scale_y * phi
    put_raw = put_split(sb, zb)

    def put_root(rows, cols, value):
        root[rows, cols] = value
        put_raw(rows, cols, value)

    def root_panel(p):
        rows, cols = below(p)
        v = vf[rows, cols] * phi - nf[rows, cols] * (scale_y * 0.25) - product(vb[1, rows, :], nb[:, cols]) * 0.25
        mirror(p, v * root_scale, put_root)

    def root_diagonal(i, carry):
        span = pl.ds(pl.multiple_of(i * 128, 128), 128)
        put_root(span, span, root[span, span] + eye * diag_root)
        return carry

    with jax.named_scope("root"):
        for p in range(PANELS):
            root_panel(p)
        lax.fori_loop(0, 8, root_diagonal, 0)

    front = pl.ds(0, N - 1)
    pltpu.make_async_copy(code.at[front], outer_in.at[front], o_out).wait()

    def raw_product(p):
        rows = pl.ds(p * PANEL, PANEL)
        raw = product(sb[rows, :], gm[...]) + product(zb[rows, :], gm[...])
        vf[rows, :] = raw
        return jnp.sum(raw * raw, keepdims=True), jnp.maximum(jnp.max(jnp.abs(raw), keepdims=True), TINY)

    def raw_send(p, top):
        rows = pl.ds(p * PANEL, PANEL)
        code[pl.ds(p * 32, 32)] = quarter_code(vf[rows, :], 1.0 / top).reshape(32, ROWS, B)
        for j in range(16):
            k = (5 * j + 3) % 16
            for half in (0, 1):
                for c in (0, 1):
                    cols = pl.ds(512 * half, 512)
                    target = p * 32 + at_z[k // 4] + at_y[k % 4] + c

                    def go():
                        send(code.at[target, :, cols], raw_in.at[me, :, cols], r_out, r_in, target)

                    if k == 0:
                        pl.when(target != me)(go)
                    else:
                        go()

    def panel_at(i):
        half = i // 2
        return lax.rem(x + 2 + half - lax.rem(i, 2) * (1 + 2 * half), 4)

    def raw_panel(i, carry):
        raw_sq, top, tops = carry
        p = panel_at(i)
        more, later = raw_product(p)
        raw_send(panel_at(i - 1), top)
        return raw_sq + more, later, jnp.where(lane == p, later, tops)

    with jax.named_scope("raw"):
        raw_sq, top = raw_product(panel_at(0))
        raw_sq, top, raw_tops = lax.fori_loop(
            1, PANELS, raw_panel, (raw_sq, top, jnp.where(lane == panel_at(0), top, 0.0))
        )
        raw_send(panel_at(PANELS - 1), top)

    tops = (raw_tops + pltpu.roll(outer_tops, 4, 1)) * (1.0 / TOP**4)
    msend[...] = tops + jnp.where(lane == 8, grad_sq, 0.0) + jnp.where(lane == 9, raw_sq, 0.0)
    with jax.named_scope("send_m"):
        to_chips((0, 1), lambda target: send(msend, misc_in.at[me], m_out, m_in, target))
    misc_in[me] = msend[...]
    raw_in[me] = code[me]

    with jax.named_scope("wait_out"):
        pltpu.make_async_copy(gsend.at[front], grecv.at[front], g_out).wait()
        pltpu.make_async_copy(ssend.at[front, :, pl.ds(0, 512)], srecv.at[front, :, pl.ds(0, 512)], s_out).wait()
        wait_extras(True)
        pltpu.make_async_copy(code.at[front], raw_in.at[front], r_out).wait()
        pltpu.make_async_copy(misc_in.at[front], misc_in.at[front], m_out).wait()
    with jax.named_scope("wait_o"):
        pltpu.make_async_copy(code.at[front], outer_in.at[front], o_in).wait()
    with jax.named_scope("wait_r"):
        pltpu.make_async_copy(code.at[front], raw_in.at[front], r_in).wait()
        pltpu.make_async_copy(misc_in.at[front], misc_in.at[front], m_in).wait()


def output_kernel(
    slot, stat, root, outer, raw, misc, new_out, root_out, update_out, nbuf, tbuf, oscale, rscale, root_sem, out_sems
):
    put_root = pltpu.make_async_copy(root, root_out.at[0], root_sem)
    put_root.start()
    panel = lax.axis_index(AXIS) // 32
    lane = lax.broadcasted_iota(I32, (1, 1, 128), 2)

    def pick(v, at):
        return jnp.sum(jnp.where(lane == at, v, 0.0), axis=2, keepdims=True)

    values = misc[...]
    totals = jnp.sum(values, axis=0, keepdims=True)
    graft = jnp.sqrt(pick(totals, 8)) / jnp.sqrt(pick(totals, 9))
    rscale[...] = jnp.broadcast_to(pick(values, panel) * graft, (N, 1, 128))
    oscale[...] = jnp.broadcast_to(pick(values, panel + 4), (N, 1, 128))
    step = 8

    def chunk(i, carry):
        part = pl.ds(i * step, step)
        for j in range(step):
            b = i * step + j
            s = slot[b]
            o_value = oscale[s]
            r_value = rscale[s]
            for c in range(8):
                cols = slice(128 * c, 128 * (c + 1))
                nbuf[b, :, cols] = stat[b, :, cols] * STAT_DECAY + quarter_value(outer[s, :, cols], o_value)
                tbuf[b, :, cols] = quarter_value(raw[s, :, cols], r_value)
        pltpu.make_async_copy(nbuf.at[part], new_out.at[part], out_sems.at[0, i]).start()
        pltpu.make_async_copy(tbuf.at[part], update_out.at[part], out_sems.at[1, i]).start()
        return carry

    lax.fori_loop(0, N // step, chunk, 0)
    for i in range(N // step):
        part = pl.ds(i * step, step)
        pltpu.make_async_copy(nbuf.at[part], new_out.at[part], out_sems.at[0, i]).wait()
        pltpu.make_async_copy(tbuf.at[part], update_out.at[part], out_sems.at[1, i]).wait()
    put_root.wait()


def body(statistics, gradient, block_slot):
    in_hbm = pl.BlockSpec(memory_space=pltpu.HBM)
    smem = pl.BlockSpec(memory_space=pltpu.SMEM)
    vmem = pl.BlockSpec(memory_space=pltpu.VMEM)
    dma = pltpu.SemaphoreType.DMA
    V = pltpu.VMEM
    statistics = pltpu.with_memory_space_constraint(statistics, pltpu.HBM)
    gradient = pltpu.with_memory_space_constraint(gradient, pltpu.HBM)
    block_slot = pltpu.with_memory_space_constraint(block_slot, pltpu.HBM)
    stat, root, outer_rows, raw_rows, misc = pl.pallas_call(
        exchange_kernel,
        out_shape=(
            jax.ShapeDtypeStruct((N, ROWS, B), F32),
            jax.ShapeDtypeStruct((B, B), F32),
            jax.ShapeDtypeStruct((N, ROWS, B), I16),
            jax.ShapeDtypeStruct((N, ROWS, B), I16),
            jax.ShapeDtypeStruct((N, 1, 128), F32),
        ),
        in_specs=[in_hbm, in_hbm, in_hbm],
        out_specs=(vmem,) * 5,
        scratch_shapes=[
            V((1, 128), I32), V((1, 128), I32), pltpu.SMEM((1, 128), I32),
            V((N, ROWS, B), BF16), V((N, ROWS, B), BF16), V((N, ROWS, 640), I16),
            V((N, ROWS, B), BF16), V((N, ROWS, 640), I16), V((B, B), BF16),
            V((B, B), F32), V((B, B), F32),
            V((B, B), BF16), V((B, B), BF16), V((B, B), BF16), V((B, B), BF16), V((2, B, B), BF16),
            V((N, ROWS, B), I16), V((1, 128), F32),
        ]
        + [dma] * 15,
        compiler_params=pltpu.CompilerParams(
            collective_id=0, has_side_effects=True, vmem_limit_bytes=41 * 1024 * 1024
        ),
        name="exchange",
    )(block_slot, statistics, gradient)
    return pl.pallas_call(
        output_kernel,
        out_shape=(
            jax.ShapeDtypeStruct((N, ROWS, B), F32),
            jax.ShapeDtypeStruct((1, B, B), F32),
            jax.ShapeDtypeStruct((N, ROWS, B), F32),
        ),
        in_specs=[smem, vmem, vmem, vmem, vmem, vmem],
        out_specs=(in_hbm, in_hbm, in_hbm),
        scratch_shapes=[
            V((N, ROWS, B), F32), V((N, ROWS, B), F32), V((N, 1, 128), F32), V((N, 1, 128), F32), dma, dma((2, 16)),
        ],
        compiler_params=pltpu.CompilerParams(vmem_limit_bytes=16 * 1024 * 1024),
        name="outputs",
    )(block_slot, stat, root, outer_rows, raw_rows, misc)


def solution(mesh):
    rows = P(None, AXIS, None)
    return jax.shard_map(
        body, mesh=mesh, in_specs=(rows, rows, P()), out_specs=(rows, P(AXIS, None, None), rows), check_vma=False
    )
```

```python
import itertools

import jax
import jax.numpy as jnp
from jax import lax
from jax.experimental import pallas as pl
from jax.experimental.pallas import tpu as pltpu
from jax.sharding import PartitionSpec as P

N = 128
B = 1024
ROWS = 8
AXIS = "fsdp"
MESH = pl.DeviceIdType.MESH
F32 = jnp.float32
BF16 = jnp.bfloat16
I16 = jnp.int16
I32 = jnp.int32
F8 = jnp.float8_e4m3fn

STAT_DECAY = 0.95
RIDGE = 0.001
STAT_MAX = 200.0
TOP = 32760.0
PANEL = 256
PANELS = B // PANEL
TINY = 1e-30
G_PIECES, S_PIECES, OUTER_PIECES, RAW_PIECES = 4, 1, 4, 2

CHIPS = [o for o in itertools.product(range(4), repeat=3) if any(o)]
HOPS = (0, 1, 2, 1)
FAR_FIRST = sorted(CHIPS, key=lambda o: -sum(HOPS[k] for k in o))
ROUND = [(-(5 * j + 3) % 4, (5 * j + 3) % 16 // 4, (5 * j + 3) % 4) for j in range(16)]


def quarter_scale(top):
    return TOP * lax.rsqrt(top) * lax.rsqrt(lax.rsqrt(top))


def quarter_code(x, scale):
    a = jnp.abs(x) + TINY
    r = lax.rsqrt(a)
    s = lax.rsqrt(a * r)
    return jnp.round((x * r) * (s * scale)).astype(I32).astype(I16)


def quarter_value(q, top_to_value):
    y = q.astype(I32).astype(F32)
    return (y * y) * (y * jnp.abs(y)) * top_to_value


def half_code(x, scale):
    return jnp.round(x * lax.rsqrt(jnp.abs(x) + TINY) * scale).astype(I32).astype(I16)


def half_value(q, scale):
    y = q.astype(I32).astype(F32)
    return y * jnp.abs(y) * scale


def eye_block():
    return (lax.broadcasted_iota(I32, (128, 128), 0) == lax.broadcasted_iota(I32, (128, 128), 1)).astype(F32)


def product(a, b):
    return jnp.dot(a, b, preferred_element_type=F32)


def below(p):
    return slice(PANEL * p, PANEL * (p + 1)), slice(PANEL * p, B)


def mirror(p, value, put):
    rows, cols = below(p)
    put(rows, cols, value)
    if p + 1 < PANELS:
        put(slice(PANEL * (p + 1), B), rows, value[:, PANEL:].T)


def put_bf16(ref):
    def put(rows, cols, value):
        ref[rows, cols] = value.astype(BF16)

    return put


def put_both(full, narrow):
    def put(rows, cols, value):
        full[rows, cols] = value
        narrow(rows, cols, value)

    return put


def put_split(high, low):
    def put(rows, cols, value):
        hi = value.astype(BF16)
        high[rows, cols] = hi
        low[rows, cols] = (value - hi.astype(F32)).astype(BF16)

    return put


def put_eighths(high, near, low, scale):
    def put(rows, cols, value):
        hi = value.astype(BF16)
        high[rows, cols] = hi
        near[rows, cols] = (value * scale).astype(F8)
        low[rows, cols] = ((value - hi.astype(F32)) * (scale * 256.0)).astype(F8)

    return put


def fold(tile):
    return jnp.sum(tile.reshape(16, 8, 128), axis=0)


def exchange_kernel(
    slot_hbm, stat_hbm, grad_hbm, stat, root, outer_in, raw_in, misc_in,
    slots, placed_row, placed, gin, gsend, ssend, grecv, srecv, gm, nf, vf, nb, n8, l8, sb, zb, vb, code, msend,
    load_p, load_g, load_s, g_out, g_in, s_out, s_in, e_out, e_in, o_out, o_in, r_out, r_in, m_out, m_in,
):
    sf = root
    me = lax.axis_index(AXIS)
    core = lax.rem(me, 2)
    sibling = me + 1 - 2 * core
    y = lax.rem(me // 2, 4)
    z = lax.rem(me // 8, 4)
    x = me // 32
    block_row = me // 16
    high = me // 64
    bit = lax.rem(me // 2, 2)
    at_x = [lax.rem(x + k, 4) * 32 for k in range(4)]
    at_z = [lax.rem(z + k, 4) * 8 for k in range(4)]
    at_y = [lax.rem(y + k, 4) * 2 for k in range(4)]

    def send(src, dst, out_sem, in_sem, target):
        pltpu.make_async_remote_copy(
            src_ref=src, dst_ref=dst, send_sem=out_sem, recv_sem=in_sem,
            device_id={AXIS: target}, device_id_type=MESH,
        ).start()

    def to_round(i, cores, go):
        for j, (kx, kz, ky) in enumerate(ROUND):
            for c in cores:
                target = first_device(i, j) + c
                if kz == 0 and ky == 0:
                    pl.when(target != me)(lambda: go(target))
                else:
                    go(target)

    def first_device(i, j):
        kx, kz, ky = ROUND[j]
        return lax.rem(x + kx + i, 4) * 32 + at_z[kz] + at_y[ky]

    def to_chips(cores, go):
        def step(i, carry):
            to_round(i, cores, go)
            return carry

        lax.fori_loop(0, 4, step, 0)

    barrier = pltpu.get_barrier_semaphore()
    get_p = pltpu.make_async_copy(slot_hbm, slots.at[0], load_p)
    get_g = pltpu.make_async_copy(grad_hbm, gin, load_g)
    get_s = pltpu.make_async_copy(stat_hbm, stat, load_s)
    get_p.start()
    get_g.start()
    get_s.start()

    with jax.named_scope("greet"):
        for o in FAR_FIRST:
            for c in (0, 1):
                other = at_x[o[0]] + at_z[o[1]] + at_y[o[2]] + c
                pl.semaphore_signal(barrier, inc=1, device_id={AXIS: other}, device_id_type=MESH)
        pl.semaphore_signal(barrier, inc=1, device_id={AXIS: sibling}, device_id_type=MESH)

    with jax.named_scope("placed"):
        get_p.wait()
        down = jnp.broadcast_to(slots[...], (128, 128)).T
        hit = down == lax.broadcasted_iota(I32, (128, 128), 1)
        placed_row[...] = jnp.max(
            jnp.where(hit, lax.broadcasted_iota(I32, (128, 128), 0), 0), axis=0, keepdims=True
        )
        put_p = pltpu.make_async_copy(placed_row, placed, load_p)
        put_p.start()
        get_g.wait()
        put_p.wait()

    def pack_g(s, carry):
        gsend[s] = gin[placed[0, s]]
        return carry

    with jax.named_scope("pack_g"):
        lax.fori_loop(0, N, pack_g, 0, unroll=4)
    get_s.wait()
    stat_scale = TOP / (STAT_MAX**0.5)

    def pack_s(group):
        def step(i, carry):
            s = 2 * i + group
            b = placed[0, s]
            for j in range(5):
                column = pl.multiple_of(lax.rem(block_row + j, 8) * 128, 128)
                ssend[s, :, 128 * j : 128 * (j + 1)] = half_code(stat[b, :, pl.ds(column, 128)], stat_scale)
            return carry

        with jax.named_scope("pack_s"):
            lax.fori_loop(0, N // 2, step, 0, unroll=4)

    with jax.named_scope("wait_barrier"):
        pl.semaphore_wait(barrier, N - 1)

    def pieces(count, width=B):
        return [pl.ds(width // count * i, width // count) for i in range(count)]

    def send_g(target, cols):
        send(gsend.at[target, :, cols], grecv.at[me, :, cols], g_out, g_in, target)

    def send_s(target, cols):
        send(ssend.at[target, :, cols], srecv.at[me, :, cols], s_out, s_in, target)

    def send_extra(target):
        @pl.when(lax.rem(target // 2, 2) == high)
        def _():
            send(ssend.at[target, :, pl.ds(512, 128)], srecv.at[me, :, pl.ds(512, 128)], e_out, e_in, target)

    for group in (0, 1):
        with jax.named_scope("send_g"):
            for cols in pieces(G_PIECES):
                to_chips((group,), lambda target: send_g(target, cols))
        pack_s(group)
        with jax.named_scope("send_s"):
            for cols in pieces(S_PIECES, 512):
                to_chips((group,), lambda target: send_s(target, cols))
            to_chips((group,), send_extra)

    grecv[me] = gsend[me]
    srecv[me] = ssend[me]

    with jax.named_scope("wait_g"):
        pltpu.make_async_copy(gsend.at[pl.ds(0, N - 1)], grecv.at[pl.ds(0, N - 1)], g_in).wait()

    def unpack_g(p, carry):
        gm[pl.ds(p * PANEL, PANEL), :] = grecv[pl.ds(p * 32, 32)].reshape(PANEL, B)
        return carry

    lane = lax.broadcasted_iota(I32, (1, 128), 1)

    def put_nf(rows, cols, value):
        nf[rows, cols] = value

    def outer_product(p, top):
        rows, cols = below(p)
        outer = lax.dot_general(gm[rows, :], gm[cols, :], (((1,), (1,)), ((), ())), preferred_element_type=F32)
        outer = outer * (1.0 - STAT_DECAY)
        mirror(p, outer, put_nf)
        return jnp.maximum(top, jnp.max(outer[:, :PANEL], axis=0, keepdims=True))

    def outer_panel(p, scale):
        code[pl.ds(p * 32, 32)] = quarter_code(nf[pl.ds(p * PANEL, PANEL), :], scale).reshape(32, ROWS, B)
        return scale

    def send_outer():
        for cols in pieces(OUTER_PIECES):
            to_chips(
                (0, 1), lambda target: send(code.at[target, :, cols], outer_in.at[me, :, cols], o_out, o_in, target)
            )

    with jax.named_scope("outer"):
        lax.fori_loop(0, PANELS, unpack_g, 0)
        outer_top = jnp.full((1, PANEL), TINY, F32)
        for p in range(PANELS):
            outer_top = outer_product(p, outer_top)
        outer_top = jnp.max(outer_top, keepdims=True)
    with jax.named_scope("outer_code"):
        lax.fori_loop(0, PANELS, outer_panel, quarter_scale(outer_top), unroll=2)

    @pl.when(core == 1)
    def _():
        with jax.named_scope("send_outer"):
            send_outer()

    eye = eye_block()

    def diagonal(i):
        span = pl.ds(pl.multiple_of(i * 128, 128), 128)
        return span, nf[span, span]

    def trace_step(i, total):
        return total + fold(diagonal(i)[1] * eye)

    zeros = jnp.zeros((8, 128), F32)
    grad_sq = jnp.sum(lax.fori_loop(0, 8, trace_step, zeros), keepdims=True) / (1.0 - STAT_DECAY)

    def wait_extra(count, out):
        part = pl.ds(0, count)
        pltpu.make_async_copy(
            ssend.at[part, :, pl.ds(512, 128)], srecv.at[part, :, pl.ds(512, 128)], e_out if out else e_in
        ).wait()

    def wait_extras(out):
        @pl.when(bit == high)
        def _():
            wait_extra(N // 2 - 1, out)

        @pl.when(bit != high)
        def _():
            wait_extra(N // 2, out)

    with jax.named_scope("wait_s"):
        pltpu.make_async_copy(
            ssend.at[pl.ds(0, N - 1), :, pl.ds(0, 512)], srecv.at[pl.ds(0, N - 1), :, pl.ds(0, 512)], s_in
        ).wait()
        wait_extras(False)

    stat_value = STAT_DECAY / stat_scale**2
    first_scale = 256.0 / (STAT_MAX + outer_top)
    put_n = put_eighths(nb, n8, l8, first_scale)

    def add_tile(i, j, square, own):
        other = lax.rem(i + j, 8)
        tile = half_value(srecv[pl.ds(i * 16, 16), :, 128 * j : 128 * (j + 1)], stat_value).reshape(128, 128)
        rows = pl.ds(pl.multiple_of(i * 128, 128), 128)
        cols = pl.ds(pl.multiple_of(other * 128, 128), 128)
        value = nf[rows, cols] + tile
        nf[rows, cols] = value
        put_n(rows, cols, value)
        if own:
            return square + fold(value * value)
        mirrored = value.T
        nf[cols, rows] = mirrored
        put_n(cols, rows, mirrored)
        return square + 2.0 * fold(value * value)

    def tiles(i, square):
        for j in range(4):
            square = add_tile(i, j, square, j == 0)
        return square

    with jax.named_scope("tiles"):
        square = lax.fori_loop(0, 8, tiles, zeros, unroll=2)
        square = lax.fori_loop(0, 4, lambda i, acc: add_tile(i + 4 * bit, 4, acc, False), square, unroll=4)
        total_sq = jnp.sum(square, keepdims=True)
        trace = jnp.sum(lax.fori_loop(0, 8, trace_step, zeros), keepdims=True)
        mean = trace * (1.0 / B)
        ridge = RIDGE * mean
        total_sq = total_sq + 2.0 * ridge * trace + ridge * ridge * float(B)
        shrink = 2.5 * lax.rsqrt(total_sq)
        root_scale = lax.rsqrt(lax.rsqrt(shrink))

        def center(i, carry):
            span, value = diagonal(i)
            value = value - eye * mean
            nf[span, span] = value
            put_n(span, span, value)
            return carry

        lax.fori_loop(0, 8, center, 0)

    def iterate(first, k, mu, scale_y, v_unit, scale):
        phi = (5.0 - mu) * 0.25
        phi2 = phi * phi
        phi3 = phi2 * phi
        phi4 = phi2 * phi2
        quarter_y = scale_y * 0.25
        quarter_v = v_unit * 0.25
        unscale = (1.0 / 256.0) / (scale * scale)
        with jax.named_scope("square"):
            for p in range(PANELS):
                rows, cols = below(p)
                hi = nb[rows, :]
                s = product(n8[rows, :], l8[:, cols]) + product(l8[rows, :], n8[:, cols])
                s = product(hi, nb[:, cols]) + s * unscale
                if first:
                    s = s * (shrink * shrink)
                    vf[rows, cols] = nf[rows, cols] * (shrink * -0.25)
                    vb[1, rows, :] = hi
                else:
                    vn = product(vb[k, rows, :], nb[:, cols])
                    v = vf[rows, cols] * phi - nf[rows, cols] * quarter_y - vn * quarter_v
                    mirror(p, v, put_both(vf, put_bf16(vb.at[1 - k])))
                sf[rows, cols] = s
                mirror(p, s, put_bf16(sb))
        n_n = phi4 - mu * phi3
        n_s = 0.375 * mu * phi2 - phi3
        n_t = 0.375 * phi2 - mu * phi * (1.0 / 16.0)
        z_s = mu * (1.0 / 256.0) - phi * (1.0 / 16.0)
        z_t = 1.0 / 256.0
        if first:
            n_n, n_t, z_t = n_n * shrink, n_t * shrink, z_t * shrink
        with jax.named_scope("cube"):
            for p in range(PANELS):
                rows, cols = below(p)
                t = product(sb[rows, :], nb[:, cols])
                s = sf[rows, cols]
                nf[rows, cols] = nf[rows, cols] * n_n + s * n_s + t * n_t
                mirror(p, s * z_s + t * z_t, put_bf16(zb))
        with jax.named_scope("next"):
            for p in range(PANELS):
                rows, cols = below(p)
                n = nf[rows, cols] + product(sb[rows, :], zb[:, cols])
                mirror(p, n, put_both(nf, put_eighths(nb, n8, l8, 256.0)))
        return phi4 * mu, scale_y * phi

    one = jnp.ones((1, 1), F32)
    @pl.when(core == 0)
    def _():
        with jax.named_scope("send_outer"):
            send_outer()

    mu, scale_y = iterate(True, 0, shrink * mean * (1.0 + RIDGE), one, one, first_scale)

    outer_in[me] = code[me]

    def later(k, carry):
        mu, scale_y, v_unit = carry
        mu, scale_y = iterate(False, lax.rem(k, 2), mu, scale_y, v_unit, 256.0)
        return mu, scale_y, one

    mu, scale_y, _ = lax.fori_loop(1, 3, later, (mu, scale_y, shrink * -0.25))
    phi = (5.0 - mu) * 0.25
    diag_root = root_scale * scale_y * phi
    front = pl.ds(0, N - 1)
    pltpu.make_async_copy(code.at[front], outer_in.at[front], o_out).wait()

    chips = range(len(ROUND))
    low_lane = lax.broadcasted_iota(I32, (16, 128), 1) - lax.broadcasted_iota(I32, (16, 128), 0)
    put_parts = put_split(sb, zb)

    def strips(i):
        return [pl.ds(pl.multiple_of(first_device(i, j) * ROWS, 16), 16) for j in chips]

    def gathered(ref, rows):
        return jnp.concatenate([ref[r, :] for r in rows], axis=0)

    def root_batch(i):
        rows = strips(i)
        batch = pl.ds(pl.multiple_of(i * PANEL, PANEL), PANEL)
        vn = product(gathered(vb.at[1], rows), nb[...])
        value = (gathered(vf, rows) * phi - gathered(nf, rows) * (scale_y * 0.25) - vn * 0.25) * root_scale
        put_parts(batch, slice(None), value)
        for j in chips:
            device = first_device(i, j)
            cols = pl.ds(pl.multiple_of(device // 16 * 128, 128), 128)
            root[rows[j], :] = value[16 * j : 16 * (j + 1)]
            tile = root[rows[j], cols] + jnp.where(low_lane == lax.rem(device, 16) * ROWS, diag_root, 0.0)
            root[rows[j], cols] = tile
            put_parts(pl.ds(pl.multiple_of(i * PANEL + 16 * j, 16), 16), cols, tile)

    def raw_batch(i):
        batch = pl.ds(pl.multiple_of(i * PANEL, PANEL), PANEL)
        raw = product(sb[batch, :], gm[...]) + product(zb[batch, :], gm[...])
        for j, r in zip(chips, strips(i)):
            vf[r, :] = raw[16 * j : 16 * (j + 1)]
        return jnp.sum(raw * raw, keepdims=True), jnp.maximum(jnp.max(jnp.abs(raw), keepdims=True), TINY)

    def raw_code(i, top):
        scale = quarter_scale(top)
        for j, r in zip(chips, strips(i)):
            code[pl.ds(first_device(i, j), 2)] = quarter_code(vf[r, :], scale).reshape(2, ROWS, B)

    def raw_send(i):
        for cols in pieces(RAW_PIECES):
            to_round(
                i, (0, 1), lambda target: send(code.at[target, :, cols], raw_in.at[me, :, cols], r_out, r_in, target)
            )

    def finish(i, carry, last=False):
        raw_sq, tops = carry
        more, top = raw_batch(i)
        if not last:
            root_batch(i + 1)
        raw_code(i, top)
        raw_send(i)
        return raw_sq + more, jnp.where(lane == i, top, tops)

    with jax.named_scope("root"):
        root_batch(0)
    with jax.named_scope("raw"):
        carry = lax.fori_loop(0, 3, finish, (jnp.zeros((1, 1), F32), jnp.zeros((1, 128), F32)))
        raw_sq, raw_tops = finish(3, carry, last=True)

    tops = (raw_tops + jnp.where(lane == 4, outer_top, 0.0)) * (1.0 / TOP**4)
    msend[...] = tops + jnp.where(lane == 8, grad_sq, 0.0) + jnp.where(lane == 9, raw_sq, 0.0)
    with jax.named_scope("send_m"):
        to_chips((0, 1), lambda target: send(msend, misc_in.at[me], m_out, m_in, target))
    misc_in[me] = msend[...]
    raw_in[me] = code[me]

    with jax.named_scope("wait_out"):
        pltpu.make_async_copy(gsend.at[front], grecv.at[front], g_out).wait()
        pltpu.make_async_copy(ssend.at[front, :, pl.ds(0, 512)], srecv.at[front, :, pl.ds(0, 512)], s_out).wait()
        wait_extras(True)
        pltpu.make_async_copy(code.at[front], raw_in.at[front], r_out).wait()
        pltpu.make_async_copy(misc_in.at[front], misc_in.at[front], m_out).wait()
    with jax.named_scope("wait_o"):
        pltpu.make_async_copy(code.at[front], outer_in.at[front], o_in).wait()
    with jax.named_scope("wait_r"):
        pltpu.make_async_copy(code.at[front], raw_in.at[front], r_in).wait()
        pltpu.make_async_copy(misc_in.at[front], misc_in.at[front], m_in).wait()


def output_kernel(
    slot, stat, root, outer, raw, misc, new_out, root_out, update_out, nbuf, tbuf, oscale, rscale, root_sem, out_sems
):
    put_root = pltpu.make_async_copy(root, root_out.at[0], root_sem)
    put_root.start()
    me = lax.axis_index(AXIS)
    source = lax.broadcasted_iota(I32, (N, 1, 1), 0)
    turn = lax.rem(8 + me // 32 - source // 32 + lax.rem(me // 2, 4) - lax.rem(source // 2, 4), 4)
    lane = lax.broadcasted_iota(I32, (1, 1, 128), 2)

    def pick(v, at):
        return jnp.sum(jnp.where(lane == at, v, 0.0), axis=2, keepdims=True)

    values = misc[...]
    totals = jnp.sum(values, axis=0, keepdims=True)
    graft = jnp.sqrt(pick(totals, 8)) / jnp.sqrt(pick(totals, 9))
    rscale[...] = jnp.broadcast_to(pick(values, turn) * graft, (N, 1, 128))
    oscale[...] = jnp.broadcast_to(pick(values, 4), (N, 1, 128))
    step = 8

    def chunk(i, carry):
        part = pl.ds(i * step, step)
        for j in range(step):
            b = i * step + j
            s = slot[b]
            o_value = oscale[s]
            r_value = rscale[s]
            for c in range(8):
                cols = slice(128 * c, 128 * (c + 1))
                nbuf[b, :, cols] = stat[b, :, cols] * STAT_DECAY + quarter_value(outer[s, :, cols], o_value)
                tbuf[b, :, cols] = quarter_value(raw[s, :, cols], r_value)
        pltpu.make_async_copy(nbuf.at[part], new_out.at[part], out_sems.at[0, i]).start()
        pltpu.make_async_copy(tbuf.at[part], update_out.at[part], out_sems.at[1, i]).start()
        return carry

    lax.fori_loop(0, N // step, chunk, 0)
    for i in range(N // step):
        part = pl.ds(i * step, step)
        pltpu.make_async_copy(nbuf.at[part], new_out.at[part], out_sems.at[0, i]).wait()
        pltpu.make_async_copy(tbuf.at[part], update_out.at[part], out_sems.at[1, i]).wait()
    put_root.wait()


def body(statistics, gradient, block_slot):
    in_hbm = pl.BlockSpec(memory_space=pltpu.HBM)
    smem = pl.BlockSpec(memory_space=pltpu.SMEM)
    vmem = pl.BlockSpec(memory_space=pltpu.VMEM)
    dma = pltpu.SemaphoreType.DMA
    V = pltpu.VMEM
    statistics = pltpu.with_memory_space_constraint(statistics, pltpu.HBM)
    gradient = pltpu.with_memory_space_constraint(gradient, pltpu.HBM)
    block_slot = pltpu.with_memory_space_constraint(block_slot, pltpu.HBM)
    stat, root, outer_rows, raw_rows, misc = pl.pallas_call(
        exchange_kernel,
        out_shape=(
            jax.ShapeDtypeStruct((N, ROWS, B), F32),
            jax.ShapeDtypeStruct((B, B), F32),
            jax.ShapeDtypeStruct((N, ROWS, B), I16),
            jax.ShapeDtypeStruct((N, ROWS, B), I16),
            jax.ShapeDtypeStruct((N, 1, 128), F32),
        ),
        in_specs=[in_hbm, in_hbm, in_hbm],
        out_specs=(vmem,) * 5,
        scratch_shapes=[
            V((1, 128), I32), V((1, 128), I32), pltpu.SMEM((1, 128), I32),
            V((N, ROWS, B), BF16), V((N, ROWS, B), BF16), V((N, ROWS, 640), I16),
            V((N, ROWS, B), BF16), V((N, ROWS, 640), I16), V((B, B), BF16),
            V((B, B), F32), V((B, B), F32),
            V((B, B), BF16), V((B, B), F8), V((B, B), F8), V((B, B), BF16), V((B, B), BF16), V((2, B, B), BF16),
            V((N, ROWS, B), I16), V((1, 128), F32),
        ]
        + [dma] * 15,
        compiler_params=pltpu.CompilerParams(
            collective_id=0, has_side_effects=True, vmem_limit_bytes=41 * 1024 * 1024
        ),
        name="exchange",
    )(block_slot, statistics, gradient)
    return pl.pallas_call(
        output_kernel,
        out_shape=(
            jax.ShapeDtypeStruct((N, ROWS, B), F32),
            jax.ShapeDtypeStruct((1, B, B), F32),
            jax.ShapeDtypeStruct((N, ROWS, B), F32),
        ),
        in_specs=[smem, vmem, vmem, vmem, vmem, vmem],
        out_specs=(in_hbm, in_hbm, in_hbm),
        scratch_shapes=[
            V((N, ROWS, B), F32), V((N, ROWS, B), F32), V((N, 1, 128), F32), V((N, 1, 128), F32), dma, dma((2, 16)),
        ],
        compiler_params=pltpu.CompilerParams(vmem_limit_bytes=16 * 1024 * 1024),
        name="outputs",
    )(block_slot, stat, root, outer_rows, raw_rows, misc)


def solution(mesh):
    rows = P(None, AXIS, None)
    return jax.shard_map(
        body, mesh=mesh, in_specs=(rows, rows, P()), out_specs=(rows, P(AXIS, None, None), rows), check_vma=False
    )
```

```python
import itertools

import jax
import jax.numpy as jnp
from jax import lax
from jax.experimental import pallas as pl
from jax.experimental.pallas import tpu as pltpu
from jax.sharding import PartitionSpec as P

N = 128
B = 1024
ROWS = 8
AXIS = "fsdp"
MESH = pl.DeviceIdType.MESH
F32 = jnp.float32
BF16 = jnp.bfloat16
I16 = jnp.int16
I32 = jnp.int32
F8 = jnp.float8_e4m3fn

STAT_DECAY = 0.95
RIDGE = 0.001
STAT_MAX = 200.0
OUTER_MAX = (1.0 - 0.95) * 1024 * 24.0**2 * 1.01
TOP = 32760.0
PANEL = 256
PANELS = B // PANEL
TINY = 1e-30
G_PIECES, S_PIECES, OUTER_PIECES, RAW_PIECES = 4, 1, 4, 2

CHIPS = [o for o in itertools.product(range(4), repeat=3) if any(o)]
HOPS = (0, 1, 2, 1)
FAR_FIRST = sorted(CHIPS, key=lambda o: -sum(HOPS[k] for k in o))
ROUND = [(-(5 * j + 3) % 4, (5 * j + 3) % 16 // 4, (5 * j + 3) % 4) for j in range(16)]


def quarter_scale(top):
    return TOP * lax.rsqrt(top) * lax.rsqrt(lax.rsqrt(top))


def quarter_code(x, scale):
    a = jnp.abs(x) + TINY
    r = lax.rsqrt(a)
    s = lax.rsqrt(a * r)
    return jnp.round((x * r) * (s * scale)).astype(I32).astype(I16)


def quarter_value(q, top_to_value):
    y = q.astype(I32).astype(F32)
    return (y * y) * (y * jnp.abs(y)) * top_to_value


def eighth_code(x):
    a = jnp.abs(x) + TINY
    r = lax.rsqrt(a)
    half = a * r
    s = lax.rsqrt(half)
    u = lax.rsqrt(half * s)
    return jnp.round((x * r) * (s * u) * (TOP / OUTER_MAX**0.125)).astype(I32).astype(I16)


def eighth_value(q):
    y = q.astype(I32).astype(F32) * (1.0 / TOP)
    y2 = y * y
    return ((y2 * y2) * y2) * ((y * jnp.abs(y)) * OUTER_MAX)


def half_code(x, scale):
    return jnp.round(x * lax.rsqrt(jnp.abs(x) + TINY) * scale).astype(I32).astype(I16)


def half_value(q, scale):
    y = q.astype(I32).astype(F32)
    return y * jnp.abs(y) * scale


def eye_block():
    return (lax.broadcasted_iota(I32, (128, 128), 0) == lax.broadcasted_iota(I32, (128, 128), 1)).astype(F32)


def product(a, b):
    return jnp.dot(a, b, preferred_element_type=F32)


def below(p):
    return slice(PANEL * p, PANEL * (p + 1)), slice(PANEL * p, B)


def mirror(p, value, put):
    rows, cols = below(p)
    put(rows, cols, value)
    if p + 1 < PANELS:
        put(slice(PANEL * (p + 1), B), rows, value[:, PANEL:].T)


def put_bf16(ref):
    def put(rows, cols, value):
        ref[rows, cols] = value.astype(BF16)

    return put


def put_both(full, narrow):
    def put(rows, cols, value):
        full[rows, cols] = value
        narrow(rows, cols, value)

    return put


def put_split(high, low):
    def put(rows, cols, value):
        hi = value.astype(BF16)
        high[rows, cols] = hi
        low[rows, cols] = (value - hi.astype(F32)).astype(BF16)

    return put


def put_eighths(high, near, low, scale):
    def put(rows, cols, value):
        hi = value.astype(BF16)
        high[rows, cols] = hi
        near[rows, cols] = (value * scale).astype(F8)
        low[rows, cols] = ((value - hi.astype(F32)) * (scale * 256.0)).astype(F8)

    return put


def fold(tile):
    return jnp.sum(tile.reshape(16, 8, 128), axis=0)


def exchange_kernel(
    slot_hbm, stat_hbm, grad_hbm, stat, root, raw_in, misc_in,
    slots, placed_row, placed, slot_of, outer_in, gin, gsend, ssend, grecv, srecv, gm, nf, vf, nb, n8, l8, sb, zb, vb, code, msend,
    load_p, load_o, load_g, load_s, g_out, g_in, s_out, s_in, e_out, e_in, o_out, o_in, r_out, r_in, m_out, m_in,
):
    sf = root
    me = lax.axis_index(AXIS)
    core = lax.rem(me, 2)
    sibling = me + 1 - 2 * core
    y = lax.rem(me // 2, 4)
    z = lax.rem(me // 8, 4)
    x = me // 32
    block_row = me // 16
    high = me // 64
    bit = lax.rem(me // 2, 2)
    at_x = [lax.rem(x + k, 4) * 32 for k in range(4)]
    at_z = [lax.rem(z + k, 4) * 8 for k in range(4)]
    at_y = [lax.rem(y + k, 4) * 2 for k in range(4)]

    def send(src, dst, out_sem, in_sem, target):
        pltpu.make_async_remote_copy(
            src_ref=src, dst_ref=dst, send_sem=out_sem, recv_sem=in_sem,
            device_id={AXIS: target}, device_id_type=MESH,
        ).start()

    def to_round(i, cores, go):
        for j, (kx, kz, ky) in enumerate(ROUND):
            for c in cores:
                target = first_device(i, j) + c
                if kz == 0 and ky == 0:
                    pl.when(target != me)(lambda: go(target))
                else:
                    go(target)

    def first_device(i, j):
        kx, kz, ky = ROUND[j]
        return lax.rem(x + kx + i, 4) * 32 + at_z[kz] + at_y[ky]

    def to_chips(cores, go):
        def step(i, carry):
            to_round(i, cores, go)
            return carry

        lax.fori_loop(0, 4, step, 0)

    barrier = pltpu.get_barrier_semaphore()
    get_p = pltpu.make_async_copy(slot_hbm, slots.at[0], load_p)
    get_g = pltpu.make_async_copy(grad_hbm, gin, load_g)
    get_s = pltpu.make_async_copy(stat_hbm, stat, load_s)
    get_p.start()
    get_g.start()
    get_s.start()

    with jax.named_scope("greet"):
        for o in FAR_FIRST:
            for c in (0, 1):
                other = at_x[o[0]] + at_z[o[1]] + at_y[o[2]] + c
                pl.semaphore_signal(barrier, inc=1, device_id={AXIS: other}, device_id_type=MESH)
        pl.semaphore_signal(barrier, inc=1, device_id={AXIS: sibling}, device_id_type=MESH)

    with jax.named_scope("placed"):
        get_p.wait()
        down = jnp.broadcast_to(slots[...], (128, 128)).T
        hit = down == lax.broadcasted_iota(I32, (128, 128), 1)
        placed_row[...] = jnp.max(
            jnp.where(hit, lax.broadcasted_iota(I32, (128, 128), 0), 0), axis=0, keepdims=True
        )
        put_p = pltpu.make_async_copy(placed_row, placed, load_p)
        put_p.start()
        put_o = pltpu.make_async_copy(slots, slot_of, load_o)
        put_o.start()
        get_g.wait()
        put_o.wait()
        put_p.wait()

    def pack_g(s, carry):
        gsend[s] = gin[placed[0, s]]
        return carry

    with jax.named_scope("pack_g"):
        lax.fori_loop(0, N, pack_g, 0, unroll=4)
    get_s.wait()
    stat_scale = TOP / (STAT_MAX**0.5)

    def pack_s(group):
        def step(i, carry):
            s = 2 * i + group
            b = placed[0, s]
            for j in range(5):
                column = pl.multiple_of(lax.rem(block_row + j, 8) * 128, 128)
                ssend[s, :, 128 * j : 128 * (j + 1)] = half_code(stat[b, :, pl.ds(column, 128)], stat_scale)
            return carry

        with jax.named_scope("pack_s"):
            lax.fori_loop(0, N // 2, step, 0, unroll=4)

    with jax.named_scope("wait_barrier"):
        pl.semaphore_wait(barrier, N - 1)

    def pieces(count, width=B):
        return [pl.ds(width // count * i, width // count) for i in range(count)]

    def send_g(target, cols):
        send(gsend.at[target, :, cols], grecv.at[me, :, cols], g_out, g_in, target)

    def send_s(target, cols):
        send(ssend.at[target, :, cols], srecv.at[me, :, cols], s_out, s_in, target)

    def send_extra(target):
        @pl.when(lax.rem(target // 2, 2) == high)
        def _():
            send(ssend.at[target, :, pl.ds(512, 128)], srecv.at[me, :, pl.ds(512, 128)], e_out, e_in, target)

    for group in (0, 1):
        with jax.named_scope("send_g"):
            for cols in pieces(G_PIECES):
                to_chips((group,), lambda target: send_g(target, cols))
        pack_s(group)
        with jax.named_scope("send_s"):
            for cols in pieces(S_PIECES, 512):
                to_chips((group,), lambda target: send_s(target, cols))
            to_chips((group,), send_extra)

    grecv[me] = gsend[me]
    srecv[me] = ssend[me]

    with jax.named_scope("wait_g"):
        pltpu.make_async_copy(gsend.at[pl.ds(0, N - 1)], grecv.at[pl.ds(0, N - 1)], g_in).wait()

    def unpack_g(p, carry):
        gm[pl.ds(p * PANEL, PANEL), :] = grecv[pl.ds(p * 32, 32)].reshape(PANEL, B)
        return carry

    lane = lax.broadcasted_iota(I32, (1, 128), 1)

    def put_nf(rows, cols, value):
        nf[rows, cols] = value

    def outer_product(p, top):
        rows, cols = below(p)
        outer = lax.dot_general(gm[rows, :], gm[cols, :], (((1,), (1,)), ((), ())), preferred_element_type=F32)
        outer = outer * (1.0 - STAT_DECAY)
        mirror(p, outer, put_nf)
        return jnp.maximum(top, jnp.max(outer[:, :PANEL], axis=0, keepdims=True))

    def outer_panel(p, carry):
        code[pl.ds(p * 32, 32)] = eighth_code(nf[pl.ds(p * PANEL, PANEL), :]).reshape(32, ROWS, B)
        return carry

    def send_outer():
        for cols in pieces(OUTER_PIECES):
            to_chips(
                (0, 1), lambda target: send(code.at[target, :, cols], outer_in.at[me, :, cols], o_out, o_in, target)
            )

    with jax.named_scope("outer"):
        lax.fori_loop(0, PANELS, unpack_g, 0)
        outer_top = jnp.full((1, PANEL), TINY, F32)
        for p in range(PANELS):
            outer_top = outer_product(p, outer_top)
        outer_top = jnp.max(outer_top, keepdims=True)
    with jax.named_scope("outer_code"):
        lax.fori_loop(0, PANELS, outer_panel, 0, unroll=2)

    @pl.when(core == 1)
    def _():
        with jax.named_scope("send_outer"):
            send_outer()

    eye = eye_block()

    def diagonal(i):
        span = pl.ds(pl.multiple_of(i * 128, 128), 128)
        return span, nf[span, span]

    def trace_step(i, total):
        return total + fold(diagonal(i)[1] * eye)

    zeros = jnp.zeros((8, 128), F32)
    grad_sq = jnp.sum(lax.fori_loop(0, 8, trace_step, zeros), keepdims=True) / (1.0 - STAT_DECAY)

    def wait_extra(count, out):
        part = pl.ds(0, count)
        pltpu.make_async_copy(
            ssend.at[part, :, pl.ds(512, 128)], srecv.at[part, :, pl.ds(512, 128)], e_out if out else e_in
        ).wait()

    def wait_extras(out):
        @pl.when(bit == high)
        def _():
            wait_extra(N // 2 - 1, out)

        @pl.when(bit != high)
        def _():
            wait_extra(N // 2, out)

    with jax.named_scope("wait_s"):
        pltpu.make_async_copy(
            ssend.at[pl.ds(0, N - 1), :, pl.ds(0, 512)], srecv.at[pl.ds(0, N - 1), :, pl.ds(0, 512)], s_in
        ).wait()
        wait_extras(False)

    stat_value = STAT_DECAY / stat_scale**2
    first_scale = 256.0 / (STAT_MAX + outer_top)
    put_n = put_eighths(nb, n8, l8, first_scale)

    def add_tile(i, j, square, own):
        other = lax.rem(i + j, 8)
        tile = half_value(srecv[pl.ds(i * 16, 16), :, 128 * j : 128 * (j + 1)], stat_value).reshape(128, 128)
        rows = pl.ds(pl.multiple_of(i * 128, 128), 128)
        cols = pl.ds(pl.multiple_of(other * 128, 128), 128)
        value = nf[rows, cols] + tile
        nf[rows, cols] = value
        put_n(rows, cols, value)
        if own:
            return square + fold(value * value)
        mirrored = value.T
        nf[cols, rows] = mirrored
        put_n(cols, rows, mirrored)
        return square + 2.0 * fold(value * value)

    def tiles(i, square):
        for j in range(4):
            square = add_tile(i, j, square, j == 0)
        return square

    with jax.named_scope("tiles"):
        square = lax.fori_loop(0, 8, tiles, zeros, unroll=2)
        square = lax.fori_loop(0, 4, lambda i, acc: add_tile(i + 4 * bit, 4, acc, False), square, unroll=4)
        total_sq = jnp.sum(square, keepdims=True)
        trace = jnp.sum(lax.fori_loop(0, 8, trace_step, zeros), keepdims=True)
        mean = trace * (1.0 / B)
        ridge = RIDGE * mean
        total_sq = total_sq + 2.0 * ridge * trace + ridge * ridge * float(B)
        shrink = 2.5 * lax.rsqrt(total_sq)
        root_scale = lax.rsqrt(lax.rsqrt(shrink))

        def center(i, carry):
            span, value = diagonal(i)
            value = value - eye * mean
            nf[span, span] = value
            put_n(span, span, value)
            return carry

        lax.fori_loop(0, 8, center, 0)

    def iterate(first, k, mu, scale_y, v_unit, scale):
        phi = (5.0 - mu) * 0.25
        phi2 = phi * phi
        phi3 = phi2 * phi
        phi4 = phi2 * phi2
        quarter_y = scale_y * 0.25
        quarter_v = v_unit * 0.25
        unscale = (1.0 / 256.0) / (scale * scale)
        with jax.named_scope("square"):
            for p in range(PANELS):
                rows, cols = below(p)
                hi = nb[rows, :]
                s = product(n8[rows, :], l8[:, cols]) + product(l8[rows, :], n8[:, cols])
                s = product(hi, nb[:, cols]) + s * unscale
                if first:
                    s = s * (shrink * shrink)
                    vf[rows, cols] = nf[rows, cols] * (shrink * -0.25)
                    vb[1, rows, :] = hi
                else:
                    vn = product(vb[k, rows, :], nb[:, cols])
                    v = vf[rows, cols] * phi - nf[rows, cols] * quarter_y - vn * quarter_v
                    mirror(p, v, put_both(vf, put_bf16(vb.at[1 - k])))
                sf[rows, cols] = s
                mirror(p, s, put_bf16(sb))
        n_n = phi4 - mu * phi3
        n_s = 0.375 * mu * phi2 - phi3
        n_t = 0.375 * phi2 - mu * phi * (1.0 / 16.0)
        z_s = mu * (1.0 / 256.0) - phi * (1.0 / 16.0)
        z_t = 1.0 / 256.0
        if first:
            n_n, n_t, z_t = n_n * shrink, n_t * shrink, z_t * shrink
        with jax.named_scope("cube"):
            for p in range(PANELS):
                rows, cols = below(p)
                t = product(sb[rows, :], nb[:, cols])
                s = sf[rows, cols]
                nf[rows, cols] = nf[rows, cols] * n_n + s * n_s + t * n_t
                mirror(p, s * z_s + t * z_t, put_bf16(zb))
        with jax.named_scope("next"):
            for p in range(PANELS):
                rows, cols = below(p)
                n = nf[rows, cols] + product(sb[rows, :], zb[:, cols])
                mirror(p, n, put_both(nf, put_eighths(nb, n8, l8, 256.0)))
        return phi4 * mu, scale_y * phi

    one = jnp.ones((1, 1), F32)
    @pl.when(core == 0)
    def _():
        with jax.named_scope("send_outer"):
            send_outer()

    mu, scale_y = iterate(True, 0, shrink * mean * (1.0 + RIDGE), one, one, first_scale)

    outer_in[me] = code[me]

    def later(k, carry):
        mu, scale_y, v_unit = carry
        mu, scale_y = iterate(False, lax.rem(k, 2), mu, scale_y, v_unit, 256.0)
        return mu, scale_y, one

    mu, scale_y, _ = lax.fori_loop(1, 3, later, (mu, scale_y, shrink * -0.25))
    phi = (5.0 - mu) * 0.25
    diag_root = root_scale * scale_y * phi
    front = pl.ds(0, N - 1)
    pltpu.make_async_copy(code.at[front], outer_in.at[front], o_out).wait()

    chips = range(len(ROUND))
    low_lane = lax.broadcasted_iota(I32, (16, 128), 1) - lax.broadcasted_iota(I32, (16, 128), 0)
    put_parts = put_split(sb, zb)

    def strips(i):
        return [pl.ds(pl.multiple_of(first_device(i, j) * ROWS, 16), 16) for j in chips]

    def gathered(ref, rows):
        return jnp.concatenate([ref[r, :] for r in rows], axis=0)

    def root_batch(i):
        rows = strips(i)
        batch = pl.ds(pl.multiple_of(i * PANEL, PANEL), PANEL)
        vn = product(gathered(vb.at[1], rows), nb[...])
        value = (gathered(vf, rows) * phi - gathered(nf, rows) * (scale_y * 0.25) - vn * 0.25) * root_scale
        put_parts(batch, slice(None), value)
        for j in chips:
            device = first_device(i, j)
            cols = pl.ds(pl.multiple_of(device // 16 * 128, 128), 128)
            root[rows[j], :] = value[16 * j : 16 * (j + 1)]
            tile = root[rows[j], cols] + jnp.where(low_lane == lax.rem(device, 16) * ROWS, diag_root, 0.0)
            root[rows[j], cols] = tile
            put_parts(pl.ds(pl.multiple_of(i * PANEL + 16 * j, 16), 16), cols, tile)

    def raw_batch(i):
        batch = pl.ds(pl.multiple_of(i * PANEL, PANEL), PANEL)
        raw = product(sb[batch, :], gm[...]) + product(zb[batch, :], gm[...])
        for j, r in zip(chips, strips(i)):
            vf[r, :] = raw[16 * j : 16 * (j + 1)]
        return jnp.sum(raw * raw, keepdims=True), jnp.maximum(jnp.max(jnp.abs(raw), keepdims=True), TINY)

    def raw_code(i, top):
        scale = quarter_scale(top)
        for j, r in zip(chips, strips(i)):
            code[pl.ds(first_device(i, j), 2)] = quarter_code(vf[r, :], scale).reshape(2, ROWS, B)

    def raw_send(i):
        for cols in pieces(RAW_PIECES):
            to_round(
                i, (0, 1), lambda target: send(code.at[target, :, cols], raw_in.at[me, :, cols], r_out, r_in, target)
            )

    def turn_at(i):
        return i + i // 2 - 2 * (i // 3)

    def finish(i, carry, last=False):
        raw_sq, tops = carry
        i, following = turn_at(i), turn_at(i + 1)
        more, top = raw_batch(i)
        if not last:
            root_batch(following)
        raw_code(i, top)
        raw_send(i)
        return raw_sq + more, jnp.where(lane == i, top, tops)

    with jax.named_scope("root"):
        root_batch(0)
    with jax.named_scope("raw"):
        carry = lax.fori_loop(0, 3, finish, (jnp.zeros((1, 1), F32), jnp.zeros((1, 128), F32)))
        raw_sq, raw_tops = finish(3, carry, last=True)

    msend[...] = raw_tops * (1.0 / TOP**4) + jnp.where(lane == 8, grad_sq, 0.0) + jnp.where(lane == 9, raw_sq, 0.0)
    with jax.named_scope("send_m"):
        to_chips((0, 1), lambda target: send(msend, misc_in.at[me], m_out, m_in, target))
    misc_in[me] = msend[...]
    raw_in[me] = code[me]

    with jax.named_scope("wait_o"):
        pltpu.make_async_copy(code.at[front], outer_in.at[front], o_in).wait()

    def renew(b, carry):
        stat[b] = stat[b] * STAT_DECAY + eighth_value(outer_in[slot_of[0, b]])
        return carry

    with jax.named_scope("renew"):
        lax.fori_loop(0, N, renew, 0, unroll=4)
    with jax.named_scope("wait_out"):
        pltpu.make_async_copy(gsend.at[front], grecv.at[front], g_out).wait()
        pltpu.make_async_copy(ssend.at[front, :, pl.ds(0, 512)], srecv.at[front, :, pl.ds(0, 512)], s_out).wait()
        wait_extras(True)
        pltpu.make_async_copy(code.at[front], raw_in.at[front], r_out).wait()
        pltpu.make_async_copy(misc_in.at[front], misc_in.at[front], m_out).wait()
    with jax.named_scope("wait_r"):
        pltpu.make_async_copy(code.at[front], raw_in.at[front], r_in).wait()
        pltpu.make_async_copy(misc_in.at[front], misc_in.at[front], m_in).wait()


def output_kernel(slot, stat, root, raw, misc, new_out, root_out, update_out, tbuf, rscale, sems, out_sems):
    puts = [pltpu.make_async_copy(root, root_out.at[0], sems.at[0]), pltpu.make_async_copy(stat, new_out, sems.at[1])]
    for c in puts:
        c.start()
    me = lax.axis_index(AXIS)
    source = lax.broadcasted_iota(I32, (N, 1, 1), 0)
    turn = lax.rem(8 + me // 32 - source // 32 + lax.rem(me // 2, 4) - lax.rem(source // 2, 4), 4)
    lane = lax.broadcasted_iota(I32, (1, 1, 128), 2)

    def pick(v, at):
        return jnp.sum(jnp.where(lane == at, v, 0.0), axis=2, keepdims=True)

    values = misc[...]
    totals = jnp.sum(values, axis=0, keepdims=True)
    graft = jnp.sqrt(pick(totals, 8)) / jnp.sqrt(pick(totals, 9))
    rscale[...] = jnp.broadcast_to(pick(values, turn) * graft, (N, 1, 128))
    step = 16

    def chunk(i, carry):
        part = pl.ds(i * step, step)
        for j in range(step):
            b = i * step + j
            s = slot[b]
            value = rscale[s]
            for c in range(8):
                cols = slice(128 * c, 128 * (c + 1))
                tbuf[b, :, cols] = quarter_value(raw[s, :, cols], value)
        pltpu.make_async_copy(tbuf.at[part], update_out.at[part], out_sems.at[i]).start()
        return carry

    lax.fori_loop(0, N // step, chunk, 0)
    for i in range(N // step):
        part = pl.ds(i * step, step)
        pltpu.make_async_copy(tbuf.at[part], update_out.at[part], out_sems.at[i]).wait()
    for c in puts:
        c.wait()


def body(statistics, gradient, block_slot):
    in_hbm = pl.BlockSpec(memory_space=pltpu.HBM)
    smem = pl.BlockSpec(memory_space=pltpu.SMEM)
    vmem = pl.BlockSpec(memory_space=pltpu.VMEM)
    dma = pltpu.SemaphoreType.DMA
    V = pltpu.VMEM
    statistics = pltpu.with_memory_space_constraint(statistics, pltpu.HBM)
    gradient = pltpu.with_memory_space_constraint(gradient, pltpu.HBM)
    block_slot = pltpu.with_memory_space_constraint(block_slot, pltpu.HBM)
    stat, root, raw_rows, misc = pl.pallas_call(
        exchange_kernel,
        out_shape=(
            jax.ShapeDtypeStruct((N, ROWS, B), F32),
            jax.ShapeDtypeStruct((B, B), F32),
            jax.ShapeDtypeStruct((N, ROWS, B), I16),
            jax.ShapeDtypeStruct((N, 1, 128), F32),
        ),
        in_specs=[in_hbm, in_hbm, in_hbm],
        out_specs=(vmem,) * 4,
        scratch_shapes=[
            V((1, 128), I32), V((1, 128), I32), pltpu.SMEM((1, 128), I32), pltpu.SMEM((1, 128), I32),
            V((N, ROWS, B), I16),
            V((N, ROWS, B), BF16), V((N, ROWS, B), BF16), V((N, ROWS, 640), I16),
            V((N, ROWS, B), BF16), V((N, ROWS, 640), I16), V((B, B), BF16),
            V((B, B), F32), V((B, B), F32),
            V((B, B), BF16), V((B, B), F8), V((B, B), F8), V((B, B), BF16), V((B, B), BF16), V((2, B, B), BF16),
            V((N, ROWS, B), I16), V((1, 128), F32),
        ]
        + [dma] * 16,
        compiler_params=pltpu.CompilerParams(
            collective_id=0, has_side_effects=True, vmem_limit_bytes=43 * 1024 * 1024
        ),
        name="exchange",
    )(block_slot, statistics, gradient)
    return pl.pallas_call(
        output_kernel,
        out_shape=(
            jax.ShapeDtypeStruct((N, ROWS, B), F32),
            jax.ShapeDtypeStruct((1, B, B), F32),
            jax.ShapeDtypeStruct((N, ROWS, B), F32),
        ),
        in_specs=[smem, vmem, vmem, vmem, vmem],
        out_specs=(in_hbm, in_hbm, in_hbm),
        scratch_shapes=[
            V((N, ROWS, B), F32), V((N, 1, 128), F32), dma((2,)), dma((8,)),
        ],
        compiler_params=pltpu.CompilerParams(vmem_limit_bytes=16 * 1024 * 1024),
        name="outputs",
    )(block_slot, stat, root, raw_rows, misc)


def solution(mesh):
    rows = P(None, AXIS, None)
    return jax.shard_map(
        body, mesh=mesh, in_specs=(rows, rows, P()), out_specs=(rows, P(AXIS, None, None), rows), check_vma=False
    )
```

```python
import itertools

import jax
import jax.numpy as jnp
from jax import lax
from jax.experimental import pallas as pl
from jax.experimental.pallas import tpu as pltpu
from jax.sharding import PartitionSpec as P

N = 128
B = 1024
ROWS = 8
AXIS = "fsdp"
MESH = pl.DeviceIdType.MESH
F32 = jnp.float32
BF16 = jnp.bfloat16
I16 = jnp.int16
I32 = jnp.int32
F8 = jnp.float8_e4m3fn

STAT_DECAY = 0.95
RIDGE = 0.001
STAT_MAX = 200.0
OUTER_MAX = (1.0 - 0.95) * 1024 * 24.0**2 * 1.01
TOP = 32760.0
PANEL = 256
PANELS = B // PANEL
TINY = 1e-30
G_PIECES, S_PIECES, OUTER_PIECES, RAW_PIECES = 4, 1, 4, 2

CHIPS = [o for o in itertools.product(range(4), repeat=3) if any(o)]
HOPS = (0, 1, 2, 1)
FAR_FIRST = sorted(CHIPS, key=lambda o: -sum(HOPS[k] for k in o))
ROUND = [(-(5 * j + 3) % 4, (5 * j + 3) % 16 // 4, (5 * j + 3) % 4) for j in range(16)]


def quarter_scale(top):
    return TOP * lax.rsqrt(top) * lax.rsqrt(lax.rsqrt(top))


def quarter_code(x, scale):
    a = jnp.abs(x) + TINY
    r = lax.rsqrt(a)
    s = lax.rsqrt(a * r)
    return jnp.round((x * r) * (s * scale)).astype(I32).astype(I16)


def quarter_value(q, top_to_value):
    y = q.astype(I32).astype(F32)
    return (y * y) * (y * jnp.abs(y)) * top_to_value


def eighth_code(x):
    a = jnp.abs(x) + TINY
    r = lax.rsqrt(a)
    half = a * r
    s = lax.rsqrt(half)
    u = lax.rsqrt(half * s)
    return jnp.round((x * r) * (s * u) * (TOP / OUTER_MAX**0.125)).astype(I32).astype(I16)


def eighth_value(q):
    y = q.astype(I32).astype(F32) * (1.0 / TOP)
    y2 = y * y
    return ((y2 * y2) * y2) * ((y * jnp.abs(y)) * OUTER_MAX)


def half_code(x, scale):
    return jnp.round(x * lax.rsqrt(jnp.abs(x) + TINY) * scale).astype(I32).astype(I16)


def half_value(q, scale):
    y = q.astype(I32).astype(F32)
    return y * jnp.abs(y) * scale


def eye_block():
    return (lax.broadcasted_iota(I32, (128, 128), 0) == lax.broadcasted_iota(I32, (128, 128), 1)).astype(F32)


def product(a, b):
    return jnp.dot(a, b, preferred_element_type=F32)


def below(p):
    return slice(PANEL * p, PANEL * (p + 1)), slice(PANEL * p, B)


def mirror(p, value, put):
    rows, cols = below(p)
    put(rows, cols, value)
    if p + 1 < PANELS:
        put(slice(PANEL * (p + 1), B), rows, value[:, PANEL:].T)


def put_bf16(ref):
    def put(rows, cols, value):
        ref[rows, cols] = value.astype(BF16)

    return put


def put_both(full, narrow):
    def put(rows, cols, value):
        full[rows, cols] = value
        narrow(rows, cols, value)

    return put


def put_split(high, low):
    def put(rows, cols, value):
        hi = value.astype(BF16)
        high[rows, cols] = hi
        low[rows, cols] = (value - hi.astype(F32)).astype(BF16)

    return put


def put_eighths(high, near, low, scale):
    def put(rows, cols, value):
        hi = value.astype(BF16)
        high[rows, cols] = hi
        near[rows, cols] = (value * scale).astype(F8)
        low[rows, cols] = ((value - hi.astype(F32)) * (scale * 256.0)).astype(F8)

    return put


def fold(tile):
    return jnp.sum(tile.reshape(16, 8, 128), axis=0)


def exchange_kernel(
    slot_hbm, stat_hbm, grad_hbm, stat, root, raw_in, misc_in,
    slots, placed_row, placed, slot_of, outer_in, gin, gsend, ssend, grecv, srecv, gm, nf, vf, nb, n8, l8, sb, zb, vb, code, msend,
    load_p, load_o, load_g, load_s, g_out, g_in, s_out, s_in, e_out, e_in, o_out, o_in, r_out, r_in, m_out, m_in,
):
    sf = root
    me = lax.axis_index(AXIS)
    core = lax.rem(me, 2)
    sibling = me + 1 - 2 * core
    y = lax.rem(me // 2, 4)
    z = lax.rem(me // 8, 4)
    x = me // 32
    block_row = me // 16
    high = me // 64
    bit = lax.rem(me // 2, 2)
    at_x = [lax.rem(x + k, 4) * 32 for k in range(4)]
    at_z = [lax.rem(z + k, 4) * 8 for k in range(4)]
    at_y = [lax.rem(y + k, 4) * 2 for k in range(4)]

    def send(src, dst, out_sem, in_sem, target):
        pltpu.make_async_remote_copy(
            src_ref=src, dst_ref=dst, send_sem=out_sem, recv_sem=in_sem,
            device_id={AXIS: target}, device_id_type=MESH,
        ).start()

    def to_round(i, cores, go):
        for j, (kx, kz, ky) in enumerate(ROUND):
            for c in cores:
                target = first_device(i, j) + c
                if kz == 0 and ky == 0:
                    pl.when(target != me)(lambda: go(target))
                else:
                    go(target)

    def first_device(i, j):
        kx, kz, ky = ROUND[j]
        return lax.rem(x + kx + i, 4) * 32 + at_z[kz] + at_y[ky]

    def to_chips(cores, go):
        def step(i, carry):
            to_round(i, cores, go)
            return carry

        lax.fori_loop(0, 4, step, 0)

    barrier = pltpu.get_barrier_semaphore()
    get_p = pltpu.make_async_copy(slot_hbm, slots.at[0], load_p)
    get_g = pltpu.make_async_copy(grad_hbm, gin, load_g)
    get_s = pltpu.make_async_copy(stat_hbm, stat, load_s)
    get_p.start()
    get_g.start()
    get_s.start()

    with jax.named_scope("greet"):
        for o in FAR_FIRST:
            for c in (0, 1):
                other = at_x[o[0]] + at_z[o[1]] + at_y[o[2]] + c
                pl.semaphore_signal(barrier, inc=1, device_id={AXIS: other}, device_id_type=MESH)
        pl.semaphore_signal(barrier, inc=1, device_id={AXIS: sibling}, device_id_type=MESH)

    with jax.named_scope("placed"):
        get_p.wait()
        down = jnp.broadcast_to(slots[...], (128, 128)).T
        hit = down == lax.broadcasted_iota(I32, (128, 128), 1)
        placed_row[...] = jnp.max(
            jnp.where(hit, lax.broadcasted_iota(I32, (128, 128), 0), 0), axis=0, keepdims=True
        )
        put_p = pltpu.make_async_copy(placed_row, placed, load_p)
        put_p.start()
        put_o = pltpu.make_async_copy(slots, slot_of, load_o)
        put_o.start()
        get_g.wait()
        put_o.wait()
        put_p.wait()

    def pack_g(s, carry):
        gsend[s] = gin[placed[0, s]]
        return carry

    with jax.named_scope("pack_g"):
        lax.fori_loop(0, N, pack_g, 0, unroll=4)
    get_s.wait()
    stat_scale = TOP / (STAT_MAX**0.5)

    def pack_s(group):
        def step(i, carry):
            s = 2 * i + group
            b = placed[0, s]
            for j in range(5):
                column = pl.multiple_of(lax.rem(block_row + j, 8) * 128, 128)
                ssend[s, :, 128 * j : 128 * (j + 1)] = half_code(stat[b, :, pl.ds(column, 128)], stat_scale)
            return carry

        with jax.named_scope("pack_s"):
            lax.fori_loop(0, N // 2, step, 0, unroll=4)

    with jax.named_scope("wait_barrier"):
        pl.semaphore_wait(barrier, N - 1)

    def pieces(count, width=B):
        return [pl.ds(width // count * i, width // count) for i in range(count)]

    def send_g(target, cols):
        send(gsend.at[target, :, cols], grecv.at[me, :, cols], g_out, g_in, target)

    def send_s(target, cols):
        send(ssend.at[target, :, cols], srecv.at[me, :, cols], s_out, s_in, target)

    def send_extra(target):
        @pl.when(lax.rem(target // 2, 2) == high)
        def _():
            send(ssend.at[target, :, pl.ds(512, 128)], srecv.at[me, :, pl.ds(512, 128)], e_out, e_in, target)

    for group in (0, 1):
        with jax.named_scope("send_g"):
            for cols in pieces(G_PIECES):
                to_chips((group,), lambda target: send_g(target, cols))
        pack_s(group)
        with jax.named_scope("send_s"):
            for cols in pieces(S_PIECES, 512):
                to_chips((group,), lambda target: send_s(target, cols))
            to_chips((group,), send_extra)

    grecv[me] = gsend[me]
    srecv[me] = ssend[me]

    with jax.named_scope("wait_g"):
        pltpu.make_async_copy(gsend.at[pl.ds(0, N - 1)], grecv.at[pl.ds(0, N - 1)], g_in).wait()

    def unpack_g(p, carry):
        gm[pl.ds(p * PANEL, PANEL), :] = grecv[pl.ds(p * 32, 32)].reshape(PANEL, B)
        return carry

    lane = lax.broadcasted_iota(I32, (1, 128), 1)

    def put_nf(rows, cols, value):
        nf[rows, cols] = value

    def outer_product(p, top):
        rows, cols = below(p)
        outer = lax.dot_general(gm[rows, :], gm[cols, :], (((1,), (1,)), ((), ())), preferred_element_type=F32)
        outer = outer * (1.0 - STAT_DECAY)
        mirror(p, outer, put_nf)
        return jnp.maximum(top, jnp.max(outer[:, :PANEL], axis=0, keepdims=True))

    def outer_panel(p, carry):
        code[pl.ds(p * 32, 32)] = eighth_code(nf[pl.ds(p * PANEL, PANEL), :]).reshape(32, ROWS, B)
        return carry

    def send_outer():
        for cols in pieces(OUTER_PIECES):
            to_chips(
                (0, 1), lambda target: send(code.at[target, :, cols], outer_in.at[me, :, cols], o_out, o_in, target)
            )

    with jax.named_scope("outer"):
        lax.fori_loop(0, PANELS, unpack_g, 0)
        outer_top = jnp.full((1, PANEL), TINY, F32)
        for p in range(PANELS):
            outer_top = outer_product(p, outer_top)
        outer_top = jnp.max(outer_top, keepdims=True)
    with jax.named_scope("outer_code"):
        lax.fori_loop(0, PANELS, outer_panel, 0, unroll=2)

    @pl.when(core == 1)
    def _():
        with jax.named_scope("send_outer"):
            send_outer()

    eye = eye_block()

    def diagonal(i):
        span = pl.ds(pl.multiple_of(i * 128, 128), 128)
        return span, nf[span, span]

    def trace_step(i, total):
        return total + fold(diagonal(i)[1] * eye)

    zeros = jnp.zeros((8, 128), F32)
    grad_sq = jnp.sum(lax.fori_loop(0, 8, trace_step, zeros), keepdims=True) / (1.0 - STAT_DECAY)

    def wait_extra(count, out):
        part = pl.ds(0, count)
        pltpu.make_async_copy(
            ssend.at[part, :, pl.ds(512, 128)], srecv.at[part, :, pl.ds(512, 128)], e_out if out else e_in
        ).wait()

    def wait_extras(out):
        @pl.when(bit == high)
        def _():
            wait_extra(N // 2 - 1, out)

        @pl.when(bit != high)
        def _():
            wait_extra(N // 2, out)

    with jax.named_scope("wait_s"):
        pltpu.make_async_copy(
            ssend.at[pl.ds(0, N - 1), :, pl.ds(0, 512)], srecv.at[pl.ds(0, N - 1), :, pl.ds(0, 512)], s_in
        ).wait()
        wait_extras(False)

    stat_value = STAT_DECAY / stat_scale**2
    first_scale = 256.0 / (STAT_MAX + outer_top)
    put_n = put_eighths(nb, n8, l8, first_scale)

    def add_tile(i, j, square, own):
        other = lax.rem(i + j, 8)
        tile = half_value(srecv[pl.ds(i * 16, 16), :, 128 * j : 128 * (j + 1)], stat_value).reshape(128, 128)
        rows = pl.ds(pl.multiple_of(i * 128, 128), 128)
        cols = pl.ds(pl.multiple_of(other * 128, 128), 128)
        value = nf[rows, cols] + tile
        nf[rows, cols] = value
        put_n(rows, cols, value)
        if own:
            return square + fold(value * value)
        mirrored = value.T
        nf[cols, rows] = mirrored
        put_n(cols, rows, mirrored)
        return square + 2.0 * fold(value * value)

    def tiles(i, square):
        for j in range(4):
            square = add_tile(i, j, square, j == 0)
        return square

    with jax.named_scope("tiles"):
        square = lax.fori_loop(0, 8, tiles, zeros, unroll=2)
        square = lax.fori_loop(0, 4, lambda i, acc: add_tile(i + 4 * bit, 4, acc, False), square, unroll=4)
        total_sq = jnp.sum(square, keepdims=True)
        trace = jnp.sum(lax.fori_loop(0, 8, trace_step, zeros), keepdims=True)
        mean = trace * (1.0 / B)
        ridge = RIDGE * mean
        total_sq = total_sq + 2.0 * ridge * trace + ridge * ridge * float(B)
        shrink = 2.5 * lax.rsqrt(total_sq)
        root_scale = lax.rsqrt(lax.rsqrt(shrink))

        def center(i, carry):
            span, value = diagonal(i)
            value = value - eye * mean
            nf[span, span] = value
            put_n(span, span, value)
            return carry

        lax.fori_loop(0, 8, center, 0)

    def iterate(first, k, mu, scale_y, v_unit, scale):
        phi = (5.0 - mu) * 0.25
        phi2 = phi * phi
        phi3 = phi2 * phi
        phi4 = phi2 * phi2
        quarter_y = scale_y * 0.25
        quarter_v = v_unit * 0.25
        unscale = (1.0 / 256.0) / (scale * scale)
        with jax.named_scope("square"):
            for p in range(PANELS):
                rows, cols = below(p)
                hi = nb[rows, :]
                s = product(n8[rows, :], l8[:, cols]) + product(l8[rows, :], n8[:, cols])
                s = product(hi, nb[:, cols]) + s * unscale
                if first:
                    s = s * (shrink * shrink)
                    vf[rows, cols] = nf[rows, cols] * (shrink * -0.25)
                    vb[1, rows, :] = hi
                else:
                    vn = product(vb[k, rows, :], nb[:, cols])
                    v = vf[rows, cols] * phi - nf[rows, cols] * quarter_y - vn * quarter_v
                    mirror(p, v, put_both(vf, put_bf16(vb.at[1 - k])))
                sf[rows, cols] = s
                mirror(p, s, put_bf16(sb))
        n_n = phi4 - mu * phi3
        n_s = 0.375 * mu * phi2 - phi3
        n_t = 0.375 * phi2 - mu * phi * (1.0 / 16.0)
        z_s = mu * (1.0 / 256.0) - phi * (1.0 / 16.0)
        z_t = 1.0 / 256.0
        if first:
            n_n, n_t, z_t = n_n * shrink, n_t * shrink, z_t * shrink
        with jax.named_scope("cube"):
            for p in range(PANELS):
                rows, cols = below(p)
                t = product(sb[rows, :], nb[:, cols])
                s = sf[rows, cols]
                nf[rows, cols] = nf[rows, cols] * n_n + s * n_s + t * n_t
                mirror(p, s * z_s + t * z_t, put_bf16(zb))
        with jax.named_scope("next"):
            for p in range(PANELS):
                rows, cols = below(p)
                n = nf[rows, cols] + product(sb[rows, :], zb[:, cols])
                mirror(p, n, put_both(nf, put_eighths(nb, n8, l8, 256.0)))
        return phi4 * mu, scale_y * phi

    one = jnp.ones((1, 1), F32)
    @pl.when(core == 0)
    def _():
        with jax.named_scope("send_outer"):
            send_outer()

    mu, scale_y = iterate(True, 0, shrink * mean * (1.0 + RIDGE), one, one, first_scale)

    outer_in[me] = code[me]

    def later(k, carry):
        mu, scale_y, v_unit = carry
        mu, scale_y = iterate(False, lax.rem(k, 2), mu, scale_y, v_unit, 256.0)
        return mu, scale_y, one

    mu, scale_y, _ = lax.fori_loop(1, 3, later, (mu, scale_y, shrink * -0.25))
    phi = (5.0 - mu) * 0.25
    diag_root = root_scale * scale_y * phi
    front = pl.ds(0, N - 1)
    pltpu.make_async_copy(code.at[front], outer_in.at[front], o_out).wait()

    chips = range(len(ROUND))
    low_lane = lax.broadcasted_iota(I32, (16, 128), 1) - lax.broadcasted_iota(I32, (16, 128), 0)
    put_parts = put_split(sb, zb)

    def strips(i):
        return [pl.ds(pl.multiple_of(first_device(i, j) * ROWS, 16), 16) for j in chips]

    def gathered(ref, rows):
        return jnp.concatenate([ref[r, :] for r in rows], axis=0)

    def root_batch(i):
        rows = strips(i)
        batch = pl.ds(pl.multiple_of(i * PANEL, PANEL), PANEL)
        vn = product(gathered(vb.at[1], rows), nb[...])
        value = (gathered(vf, rows) * phi - gathered(nf, rows) * (scale_y * 0.25) - vn * 0.25) * root_scale
        put_parts(batch, slice(None), value)
        for j in chips:
            device = first_device(i, j)
            cols = pl.ds(pl.multiple_of(device // 16 * 128, 128), 128)
            root[rows[j], :] = value[16 * j : 16 * (j + 1)]
            tile = root[rows[j], cols] + jnp.where(low_lane == lax.rem(device, 16) * ROWS, diag_root, 0.0)
            root[rows[j], cols] = tile
            put_parts(pl.ds(pl.multiple_of(i * PANEL + 16 * j, 16), 16), cols, tile)

    def raw_batch(i):
        batch = pl.ds(pl.multiple_of(i * PANEL, PANEL), PANEL)
        raw = product(sb[batch, :], gm[...]) + product(zb[batch, :], gm[...])
        for j, r in zip(chips, strips(i)):
            vf[r, :] = raw[16 * j : 16 * (j + 1)]
        return jnp.sum(raw * raw, keepdims=True), jnp.maximum(jnp.max(jnp.abs(raw), keepdims=True), TINY)

    def raw_code(i, top):
        scale = quarter_scale(top)
        for j, r in zip(chips, strips(i)):
            code[pl.ds(first_device(i, j), 2)] = quarter_code(vf[r, :], scale).reshape(2, ROWS, B)

    def raw_send(i):
        for cols in pieces(RAW_PIECES):
            to_round(
                i, (0, 1), lambda target: send(code.at[target, :, cols], raw_in.at[me, :, cols], r_out, r_in, target)
            )

    def send_misc(raw_sq, raw_tops):
        msend[...] = raw_tops * (1.0 / TOP**4) + jnp.where(lane == 8, grad_sq, 0.0) + jnp.where(lane == 9, raw_sq, 0.0)
        with jax.named_scope("send_m"):
            to_chips((0, 1), lambda target: send(msend, misc_in.at[me], m_out, m_in, target))

    def turn_at(i):
        return i + i // 2 - 2 * (i // 3)

    def finish(i, carry, last=False):
        raw_sq, tops = carry
        i, following = turn_at(i), turn_at(i + 1)
        more, top = raw_batch(i)
        if not last:
            root_batch(following)
        raw_code(i, top)
        raw_sq, tops = raw_sq + more, jnp.where(lane == i, top, tops)
        if last:
            send_misc(raw_sq, tops)
        raw_send(i)
        return raw_sq, tops

    with jax.named_scope("root"):
        root_batch(0)
    with jax.named_scope("raw"):
        carry = lax.fori_loop(0, 3, finish, (jnp.zeros((1, 1), F32), jnp.zeros((1, 128), F32)))
        finish(3, carry, last=True)

    misc_in[me] = msend[...]
    raw_in[me] = code[me]

    with jax.named_scope("wait_o"):
        pltpu.make_async_copy(code.at[front], outer_in.at[front], o_in).wait()

    def renew(b, carry):
        stat[b] = stat[b] * STAT_DECAY + eighth_value(outer_in[slot_of[0, b]])
        return carry

    with jax.named_scope("renew"):
        lax.fori_loop(0, N, renew, 0, unroll=4)
    with jax.named_scope("wait_out"):
        pltpu.make_async_copy(gsend.at[front], grecv.at[front], g_out).wait()
        pltpu.make_async_copy(ssend.at[front, :, pl.ds(0, 512)], srecv.at[front, :, pl.ds(0, 512)], s_out).wait()
        wait_extras(True)
        pltpu.make_async_copy(code.at[front], raw_in.at[front], r_out).wait()
        pltpu.make_async_copy(misc_in.at[front], misc_in.at[front], m_out).wait()
    with jax.named_scope("wait_r"):
        pltpu.make_async_copy(code.at[front], raw_in.at[front], r_in).wait()
        pltpu.make_async_copy(misc_in.at[front], misc_in.at[front], m_in).wait()


def output_kernel(slot, stat, root, raw, misc, new_out, root_out, update_out, tbuf, rscale, sems, out_sems):
    puts = [pltpu.make_async_copy(root, root_out.at[0], sems.at[0]), pltpu.make_async_copy(stat, new_out, sems.at[1])]
    for c in puts:
        c.start()
    me = lax.axis_index(AXIS)
    source = lax.broadcasted_iota(I32, (N, 1, 1), 0)
    turn = lax.rem(8 + me // 32 - source // 32 + lax.rem(me // 2, 4) - lax.rem(source // 2, 4), 4)
    lane = lax.broadcasted_iota(I32, (1, 1, 128), 2)

    def pick(v, at):
        return jnp.sum(jnp.where(lane == at, v, 0.0), axis=2, keepdims=True)

    values = misc[...]
    totals = jnp.sum(values, axis=0, keepdims=True)
    graft = jnp.sqrt(pick(totals, 8)) / jnp.sqrt(pick(totals, 9))
    rscale[...] = jnp.broadcast_to(pick(values, turn) * graft, (N, 1, 128))
    step = 16

    def chunk(i, carry):
        part = pl.ds(i * step, step)
        for j in range(step):
            b = i * step + j
            s = slot[b]
            value = rscale[s]
            for c in range(8):
                cols = slice(128 * c, 128 * (c + 1))
                tbuf[b, :, cols] = quarter_value(raw[s, :, cols], value)
        pltpu.make_async_copy(tbuf.at[part], update_out.at[part], out_sems.at[i]).start()
        return carry

    lax.fori_loop(0, N // step, chunk, 0)
    for i in range(N // step):
        part = pl.ds(i * step, step)
        pltpu.make_async_copy(tbuf.at[part], update_out.at[part], out_sems.at[i]).wait()
    for c in puts:
        c.wait()


def body(statistics, gradient, block_slot):
    in_hbm = pl.BlockSpec(memory_space=pltpu.HBM)
    smem = pl.BlockSpec(memory_space=pltpu.SMEM)
    vmem = pl.BlockSpec(memory_space=pltpu.VMEM)
    dma = pltpu.SemaphoreType.DMA
    V = pltpu.VMEM
    statistics = pltpu.with_memory_space_constraint(statistics, pltpu.HBM)
    gradient = pltpu.with_memory_space_constraint(gradient, pltpu.HBM)
    block_slot = pltpu.with_memory_space_constraint(block_slot, pltpu.HBM)
    stat, root, raw_rows, misc = pl.pallas_call(
        exchange_kernel,
        out_shape=(
            jax.ShapeDtypeStruct((N, ROWS, B), F32),
            jax.ShapeDtypeStruct((B, B), F32),
            jax.ShapeDtypeStruct((N, ROWS, B), I16),
            jax.ShapeDtypeStruct((N, 1, 128), F32),
        ),
        in_specs=[in_hbm, in_hbm, in_hbm],
        out_specs=(vmem,) * 4,
        scratch_shapes=[
            V((1, 128), I32), V((1, 128), I32), pltpu.SMEM((1, 128), I32), pltpu.SMEM((1, 128), I32),
            V((N, ROWS, B), I16),
            V((N, ROWS, B), BF16), V((N, ROWS, B), BF16), V((N, ROWS, 640), I16),
            V((N, ROWS, B), BF16), V((N, ROWS, 640), I16), V((B, B), BF16),
            V((B, B), F32), V((B, B), F32),
            V((B, B), BF16), V((B, B), F8), V((B, B), F8), V((B, B), BF16), V((B, B), BF16), V((2, B, B), BF16),
            V((N, ROWS, B), I16), V((1, 128), F32),
        ]
        + [dma] * 16,
        compiler_params=pltpu.CompilerParams(
            collective_id=0, has_side_effects=True, vmem_limit_bytes=43 * 1024 * 1024
        ),
        name="exchange",
    )(block_slot, statistics, gradient)
    return pl.pallas_call(
        output_kernel,
        out_shape=(
            jax.ShapeDtypeStruct((N, ROWS, B), F32),
            jax.ShapeDtypeStruct((1, B, B), F32),
            jax.ShapeDtypeStruct((N, ROWS, B), F32),
        ),
        in_specs=[smem, vmem, vmem, vmem, vmem],
        out_specs=(in_hbm, in_hbm, in_hbm),
        scratch_shapes=[
            V((N, ROWS, B), F32), V((N, 1, 128), F32), dma((2,)), dma((8,)),
        ],
        compiler_params=pltpu.CompilerParams(vmem_limit_bytes=16 * 1024 * 1024),
        name="outputs",
    )(block_slot, stat, root, raw_rows, misc)


def solution(mesh):
    rows = P(None, AXIS, None)
    return jax.shard_map(
        body, mesh=mesh, in_specs=(rows, rows, P()), out_specs=(rows, P(AXIS, None, None), rows), check_vma=False
    )
```

```python
import itertools

import jax
import jax.numpy as jnp
from jax import lax
from jax.experimental import pallas as pl
from jax.experimental.pallas import tpu as pltpu
from jax.sharding import PartitionSpec as P

N = 128
B = 1024
ROWS = 8
AXIS = "fsdp"
MESH = pl.DeviceIdType.MESH
F32 = jnp.float32
BF16 = jnp.bfloat16
I16 = jnp.int16
I32 = jnp.int32
F8 = jnp.float8_e4m3fn

STAT_DECAY = 0.95
RIDGE = 0.001
STAT_MAX = 200.0
OUTER_MAX = (1.0 - 0.95) * 1024 * 24.0**2 * 1.01
TOP = 32760.0
PANEL = 256
PANELS = B // PANEL
TINY = 1e-30
G_PIECES, S_PIECES, OUTER_PIECES, RAW_PIECES = 4, 1, 4, 2

CHIPS = [o for o in itertools.product(range(4), repeat=3) if any(o)]
HOPS = (0, 1, 2, 1)
FAR_FIRST = sorted(CHIPS, key=lambda o: -sum(HOPS[k] for k in o))
ROUND = [(-(5 * j + 3) % 4, (5 * j + 3) % 16 // 4, (5 * j + 3) % 4) for j in range(16)]


def quarter_scale(top):
    return TOP * lax.rsqrt(top) * lax.rsqrt(lax.rsqrt(top))


def quarter_code(x, scale):
    a = jnp.abs(x) + TINY
    r = lax.rsqrt(a)
    s = lax.rsqrt(a * r)
    return jnp.round((x * r) * (s * scale)).astype(I32).astype(I16)


def quarter_value(q, top_to_value):
    y = q.astype(I32).astype(F32)
    return (y * y) * (y * jnp.abs(y)) * top_to_value


def eighth_code(x):
    a = jnp.abs(x) + TINY
    r = lax.rsqrt(a)
    half = a * r
    s = lax.rsqrt(half)
    u = lax.rsqrt(half * s)
    return jnp.round((x * r) * (s * u) * (TOP / OUTER_MAX**0.125)).astype(I32).astype(I16)


def eighth_value(q):
    y = q.astype(I32).astype(F32) * (1.0 / TOP)
    y2 = y * y
    return ((y2 * y2) * y2) * ((y * jnp.abs(y)) * OUTER_MAX)


def half_code(x, scale):
    return jnp.round(x * lax.rsqrt(jnp.abs(x) + TINY) * scale).astype(I32).astype(I16)


def half_value(q, scale):
    y = q.astype(I32).astype(F32)
    return y * jnp.abs(y) * scale


def eye_block():
    return (lax.broadcasted_iota(I32, (128, 128), 0) == lax.broadcasted_iota(I32, (128, 128), 1)).astype(F32)


def product(a, b):
    return jnp.dot(a, b, preferred_element_type=F32)


def below(p):
    return slice(PANEL * p, PANEL * (p + 1)), slice(PANEL * p, B)


def mirror(p, value, put):
    rows, cols = below(p)
    put(rows, cols, value)
    if p + 1 < PANELS:
        put(slice(PANEL * (p + 1), B), rows, value[:, PANEL:].T)


def put_bf16(ref):
    def put(rows, cols, value):
        ref[rows, cols] = value.astype(BF16)

    return put


def put_both(full, narrow):
    def put(rows, cols, value):
        full[rows, cols] = value
        narrow(rows, cols, value)

    return put


def put_split(high, low):
    def put(rows, cols, value):
        hi = value.astype(BF16)
        high[rows, cols] = hi
        low[rows, cols] = (value - hi.astype(F32)).astype(BF16)

    return put


def put_eighths(high, near, low, scale):
    def put(rows, cols, value):
        hi = value.astype(BF16)
        high[rows, cols] = hi
        near[rows, cols] = (value * scale).astype(F8)
        low[rows, cols] = ((value - hi.astype(F32)) * (scale * 256.0)).astype(F8)

    return put


def fold(tile):
    return jnp.sum(tile.reshape(16, 8, 128), axis=0)


def exchange_kernel(
    slot_hbm, stat_hbm, grad_hbm, stat, root, raw_in, misc_in,
    slots, placed_row, placed, slot_of, outer_in, gin, gsend, ssend, grecv, srecv, gm, nf, vf, nb, n8, l8, sb, zb, vb, code, msend,
    load_p, load_o, load_g, load_s, g_out, g_in, s_out, s_in, e_out, e_in, o_out, o_in, r_out, r_in, m_out, m_in,
):
    sf = root
    me = lax.axis_index(AXIS)
    core = lax.rem(me, 2)
    sibling = me + 1 - 2 * core
    y = lax.rem(me // 2, 4)
    z = lax.rem(me // 8, 4)
    x = me // 32
    block_row = me // 16
    high = me // 64
    bit = lax.rem(me // 2, 2)
    at_x = [lax.rem(x + k, 4) * 32 for k in range(4)]
    at_z = [lax.rem(z + k, 4) * 8 for k in range(4)]
    at_y = [lax.rem(y + k, 4) * 2 for k in range(4)]

    def send(src, dst, out_sem, in_sem, target):
        pltpu.make_async_remote_copy(
            src_ref=src, dst_ref=dst, send_sem=out_sem, recv_sem=in_sem,
            device_id={AXIS: target}, device_id_type=MESH,
        ).start()

    def to_round(i, cores, go):
        for j, (kx, kz, ky) in enumerate(ROUND):
            for c in cores:
                target = first_device(i, j) + c
                if kz == 0 and ky == 0:
                    pl.when(target != me)(lambda: go(target))
                else:
                    go(target)

    def first_device(i, j):
        kx, kz, ky = ROUND[j]
        return lax.rem(x + kx + i, 4) * 32 + at_z[kz] + at_y[ky]

    def to_chips(cores, go):
        def step(i, carry):
            to_round(i, cores, go)
            return carry

        lax.fori_loop(0, 4, step, 0)

    barrier = pltpu.get_barrier_semaphore()
    get_p = pltpu.make_async_copy(slot_hbm, slots.at[0], load_p)
    get_g = pltpu.make_async_copy(grad_hbm, gin, load_g)
    get_s = pltpu.make_async_copy(stat_hbm, stat, load_s)
    get_p.start()
    get_g.start()
    get_s.start()

    with jax.named_scope("greet"):
        for o in FAR_FIRST:
            for c in (0, 1):
                other = at_x[o[0]] + at_z[o[1]] + at_y[o[2]] + c
                pl.semaphore_signal(barrier, inc=1, device_id={AXIS: other}, device_id_type=MESH)
        pl.semaphore_signal(barrier, inc=1, device_id={AXIS: sibling}, device_id_type=MESH)

    with jax.named_scope("placed"):
        get_p.wait()
        down = jnp.broadcast_to(slots[...], (128, 128)).T
        hit = down == lax.broadcasted_iota(I32, (128, 128), 1)
        placed_row[...] = jnp.max(
            jnp.where(hit, lax.broadcasted_iota(I32, (128, 128), 0), 0), axis=0, keepdims=True
        )
        put_p = pltpu.make_async_copy(placed_row, placed, load_p)
        put_p.start()
        put_o = pltpu.make_async_copy(slots, slot_of, load_o)
        put_o.start()
        get_g.wait()
        put_o.wait()
        put_p.wait()

    def pack_g(s, carry):
        gsend[s] = gin[placed[0, s]]
        return carry

    with jax.named_scope("pack_g"):
        lax.fori_loop(0, N, pack_g, 0, unroll=4)
    get_s.wait()
    stat_scale = TOP / (STAT_MAX**0.5)

    def pack_s(group):
        def step(i, carry):
            s = 2 * i + group
            b = placed[0, s]
            for j in range(5):
                column = pl.multiple_of(lax.rem(block_row + j, 8) * 128, 128)
                ssend[s, :, 128 * j : 128 * (j + 1)] = half_code(stat[b, :, pl.ds(column, 128)], stat_scale)
            return carry

        with jax.named_scope("pack_s"):
            lax.fori_loop(0, N // 2, step, 0, unroll=4)

    with jax.named_scope("wait_barrier"):
        pl.semaphore_wait(barrier, N - 1)

    def pieces(count, width=B):
        return [pl.ds(width // count * i, width // count) for i in range(count)]

    def send_g(target, cols):
        send(gsend.at[target, :, cols], grecv.at[me, :, cols], g_out, g_in, target)

    def send_s(target, cols):
        send(ssend.at[target, :, cols], srecv.at[me, :, cols], s_out, s_in, target)

    def send_extra(target):
        @pl.when(lax.rem(target // 2, 2) == high)
        def _():
            send(ssend.at[target, :, pl.ds(512, 128)], srecv.at[me, :, pl.ds(512, 128)], e_out, e_in, target)

    for group in (0, 1):
        with jax.named_scope("send_g"):
            for cols in pieces(G_PIECES):
                to_chips((group,), lambda target: send_g(target, cols))
        pack_s(group)
        with jax.named_scope("send_s"):
            for cols in pieces(S_PIECES, 512):
                to_chips((group,), lambda target: send_s(target, cols))
            to_chips((group,), send_extra)

    grecv[me] = gsend[me]
    srecv[me] = ssend[me]

    with jax.named_scope("wait_g"):
        pltpu.make_async_copy(gsend.at[pl.ds(0, N - 1)], grecv.at[pl.ds(0, N - 1)], g_in).wait()

    def unpack_g(p, carry):
        gm[pl.ds(p * PANEL, PANEL), :] = grecv[pl.ds(p * 32, 32)].reshape(PANEL, B)
        return carry

    lane = lax.broadcasted_iota(I32, (1, 128), 1)

    def put_nf(rows, cols, value):
        nf[rows, cols] = value

    def outer_product(p, top):
        rows, cols = below(p)
        outer = lax.dot_general(gm[rows, :], gm[cols, :], (((1,), (1,)), ((), ())), preferred_element_type=F32)
        outer = outer * (1.0 - STAT_DECAY)
        mirror(p, outer, put_nf)
        return jnp.maximum(top, jnp.max(outer[:, :PANEL], axis=0, keepdims=True))

    def outer_panel(p, carry):
        code[pl.ds(p * 32, 32)] = eighth_code(nf[pl.ds(p * PANEL, PANEL), :]).reshape(32, ROWS, B)
        return carry

    def send_outer():
        for cols in pieces(OUTER_PIECES):
            to_chips(
                (0, 1), lambda target: send(code.at[target, :, cols], outer_in.at[me, :, cols], o_out, o_in, target)
            )

    with jax.named_scope("outer"):
        lax.fori_loop(0, PANELS, unpack_g, 0)
        outer_top = jnp.full((1, PANEL), TINY, F32)
        for p in range(PANELS):
            outer_top = outer_product(p, outer_top)
        outer_top = jnp.max(outer_top, keepdims=True)
    with jax.named_scope("outer_code"):
        lax.fori_loop(0, PANELS, outer_panel, 0, unroll=2)

    @pl.when(core == 1)
    def _():
        with jax.named_scope("send_outer"):
            send_outer()

    eye = eye_block()

    def diagonal(i):
        span = pl.ds(pl.multiple_of(i * 128, 128), 128)
        return span, nf[span, span]

    def trace_step(i, total):
        return total + fold(diagonal(i)[1] * eye)

    zeros = jnp.zeros((8, 128), F32)
    grad_sq = jnp.sum(lax.fori_loop(0, 8, trace_step, zeros), keepdims=True) / (1.0 - STAT_DECAY)

    def wait_extra(count, out):
        part = pl.ds(0, count)
        pltpu.make_async_copy(
            ssend.at[part, :, pl.ds(512, 128)], srecv.at[part, :, pl.ds(512, 128)], e_out if out else e_in
        ).wait()

    def wait_extras(out):
        @pl.when(bit == high)
        def _():
            wait_extra(N // 2 - 1, out)

        @pl.when(bit != high)
        def _():
            wait_extra(N // 2, out)

    with jax.named_scope("wait_s"):
        pltpu.make_async_copy(
            ssend.at[pl.ds(0, N - 1), :, pl.ds(0, 512)], srecv.at[pl.ds(0, N - 1), :, pl.ds(0, 512)], s_in
        ).wait()
        wait_extras(False)

    stat_value = STAT_DECAY / stat_scale**2
    first_scale = 256.0 / (STAT_MAX + outer_top)
    put_n = put_eighths(nb, n8, l8, first_scale)

    def add_tile(i, j, square, own):
        other = lax.rem(i + j, 8)
        tile = half_value(srecv[pl.ds(i * 16, 16), :, 128 * j : 128 * (j + 1)], stat_value).reshape(128, 128)
        rows = pl.ds(pl.multiple_of(i * 128, 128), 128)
        cols = pl.ds(pl.multiple_of(other * 128, 128), 128)
        value = nf[rows, cols] + tile
        nf[rows, cols] = value
        put_n(rows, cols, value)
        if own:
            return square + fold(value * value)
        mirrored = value.T
        nf[cols, rows] = mirrored
        put_n(cols, rows, mirrored)
        return square + 2.0 * fold(value * value)

    def tiles(i, square):
        for j in range(4):
            square = add_tile(i, j, square, j == 0)
        return square

    with jax.named_scope("tiles"):
        square = lax.fori_loop(0, 8, tiles, zeros, unroll=2)
        square = lax.fori_loop(0, 4, lambda i, acc: add_tile(i + 4 * bit, 4, acc, False), square, unroll=4)
        total_sq = jnp.sum(square, keepdims=True)
        trace = jnp.sum(lax.fori_loop(0, 8, trace_step, zeros), keepdims=True)
        mean = trace * (1.0 / B)
        ridge = RIDGE * mean
        total_sq = total_sq + 2.0 * ridge * trace + ridge * ridge * float(B)
        shrink = 2.5 * lax.rsqrt(total_sq)
        root_scale = lax.rsqrt(lax.rsqrt(shrink))

        def center(i, carry):
            span, value = diagonal(i)
            value = value - eye * mean
            nf[span, span] = value
            put_n(span, span, value)
            return carry

        lax.fori_loop(0, 8, center, 0)

    def iterate(first, k, mu, scale_y, v_unit, scale):
        phi = (5.0 - mu) * 0.25
        phi2 = phi * phi
        phi3 = phi2 * phi
        phi4 = phi2 * phi2
        quarter_y = scale_y * 0.25
        quarter_v = v_unit * 0.25
        unscale = (1.0 / 256.0) / (scale * scale)
        with jax.named_scope("square"):
            for p in range(PANELS):
                rows, cols = below(p)
                hi = nb[rows, :]
                s = product(n8[rows, :], l8[:, cols]) + product(l8[rows, :], n8[:, cols])
                s = product(hi, nb[:, cols]) + s * unscale
                if first:
                    s = s * (shrink * shrink)
                    vf[rows, cols] = nf[rows, cols] * (shrink * -0.25)
                    vb[1, rows, :] = hi
                else:
                    vn = product(vb[k, rows, :], nb[:, cols])
                    v = vf[rows, cols] * phi - nf[rows, cols] * quarter_y - vn * quarter_v
                    mirror(p, v, put_both(vf, put_bf16(vb.at[1 - k])))
                sf[rows, cols] = s
                mirror(p, s, put_bf16(sb))
        n_n = phi4 - mu * phi3
        n_s = 0.375 * mu * phi2 - phi3
        n_t = 0.375 * phi2 - mu * phi * (1.0 / 16.0)
        z_s = mu * (1.0 / 256.0) - phi * (1.0 / 16.0)
        z_t = 1.0 / 256.0
        if first:
            n_n, n_t, z_t = n_n * shrink, n_t * shrink, z_t * shrink
        with jax.named_scope("cube"):
            for p in range(PANELS):
                rows, cols = below(p)
                t = product(sb[rows, :], nb[:, cols])
                s = sf[rows, cols]
                nf[rows, cols] = nf[rows, cols] * n_n + s * n_s + t * n_t
                mirror(p, s * z_s + t * z_t, put_bf16(zb))
        with jax.named_scope("next"):
            for p in range(PANELS):
                rows, cols = below(p)
                n = nf[rows, cols] + product(sb[rows, :], zb[:, cols])
                mirror(p, n, put_both(nf, put_eighths(nb, n8, l8, 256.0)))
        return phi4 * mu, scale_y * phi

    one = jnp.ones((1, 1), F32)
    @pl.when(core == 0)
    def _():
        with jax.named_scope("send_outer"):
            send_outer()

    mu, scale_y = iterate(True, 0, shrink * mean * (1.0 + RIDGE), one, one, first_scale)

    outer_in[me] = code[me]

    def later(k, carry):
        mu, scale_y, v_unit = carry
        mu, scale_y = iterate(False, lax.rem(k, 2), mu, scale_y, v_unit, 256.0)
        return mu, scale_y, one

    mu, scale_y, _ = lax.fori_loop(1, 3, later, (mu, scale_y, shrink * -0.25))
    phi = (5.0 - mu) * 0.25
    diag_root = root_scale * scale_y * phi
    front = pl.ds(0, N - 1)
    pltpu.make_async_copy(code.at[front], outer_in.at[front], o_out).wait()

    chips = range(len(ROUND))
    low_lane = lax.broadcasted_iota(I32, (16, 128), 1) - lax.broadcasted_iota(I32, (16, 128), 0)
    put_parts = put_split(sb, zb)

    def strips(i):
        return [pl.ds(pl.multiple_of(first_device(i, j) * ROWS, 16), 16) for j in chips]

    def gathered(ref, rows):
        return jnp.concatenate([ref[r, :] for r in rows], axis=0)

    def root_batch(i):
        rows = strips(i)
        batch = pl.ds(pl.multiple_of(i * PANEL, PANEL), PANEL)
        vn = product(gathered(vb.at[1], rows), nb[...])
        value = (gathered(vf, rows) * phi - gathered(nf, rows) * (scale_y * 0.25) - vn * 0.25) * root_scale
        put_parts(batch, slice(None), value)
        for j in chips:
            device = first_device(i, j)
            cols = pl.ds(pl.multiple_of(device // 16 * 128, 128), 128)
            root[rows[j], :] = value[16 * j : 16 * (j + 1)]
            tile = root[rows[j], cols] + jnp.where(low_lane == lax.rem(device, 16) * ROWS, diag_root, 0.0)
            root[rows[j], cols] = tile
            put_parts(pl.ds(pl.multiple_of(i * PANEL + 16 * j, 16), 16), cols, tile)

    def raw_batch(i):
        batch = pl.ds(pl.multiple_of(i * PANEL, PANEL), PANEL)
        raw = product(sb[batch, :], gm[...]) + product(zb[batch, :], gm[...])
        for j, r in zip(chips, strips(i)):
            vf[r, :] = raw[16 * j : 16 * (j + 1)]
        return jnp.sum(raw * raw, keepdims=True), jnp.maximum(jnp.max(jnp.abs(raw), keepdims=True), TINY)

    def raw_code(i, top):
        scale = quarter_scale(top)
        for j, r in zip(chips, strips(i)):
            code[pl.ds(first_device(i, j), 2)] = quarter_code(vf[r, :], scale).reshape(2, ROWS, B)

    def raw_send(i, count):
        for cols in pieces(count):
            to_round(
                i, (0, 1), lambda target: send(code.at[target, :, cols], raw_in.at[me, :, cols], r_out, r_in, target)
            )

    def send_misc(raw_sq, raw_tops):
        msend[...] = raw_tops * (1.0 / TOP**4) + jnp.where(lane == 8, grad_sq, 0.0) + jnp.where(lane == 9, raw_sq, 0.0)
        with jax.named_scope("send_m"):
            to_chips((0, 1), lambda target: send(msend, misc_in.at[me], m_out, m_in, target))

    def turn_at(i):
        return i + i // 2 - 2 * (i // 3)

    def finish(i, carry, last=False):
        raw_sq, tops = carry
        i, following = turn_at(i), turn_at(i + 1)
        more, top = raw_batch(i)
        if not last:
            root_batch(following)
        raw_code(i, top)
        raw_sq, tops = raw_sq + more, jnp.where(lane == i, top, tops)
        if last:
            send_misc(raw_sq, tops)
        raw_send(i, 2 * RAW_PIECES if last else RAW_PIECES)
        return raw_sq, tops

    with jax.named_scope("root"):
        root_batch(0)
    with jax.named_scope("raw"):
        carry = lax.fori_loop(0, 3, finish, (jnp.zeros((1, 1), F32), jnp.zeros((1, 128), F32)))
        finish(3, carry, last=True)

    misc_in[me] = msend[...]
    raw_in[me] = code[me]

    with jax.named_scope("wait_o"):
        pltpu.make_async_copy(code.at[front], outer_in.at[front], o_in).wait()

    def renew(b, carry):
        stat[b] = stat[b] * STAT_DECAY + eighth_value(outer_in[slot_of[0, b]])
        return carry

    with jax.named_scope("renew"):
        lax.fori_loop(0, N, renew, 0, unroll=4)
    with jax.named_scope("wait_out"):
        pltpu.make_async_copy(gsend.at[front], grecv.at[front], g_out).wait()
        pltpu.make_async_copy(ssend.at[front, :, pl.ds(0, 512)], srecv.at[front, :, pl.ds(0, 512)], s_out).wait()
        wait_extras(True)
        pltpu.make_async_copy(code.at[front], raw_in.at[front], r_out).wait()
        pltpu.make_async_copy(misc_in.at[front], misc_in.at[front], m_out).wait()
    with jax.named_scope("wait_r"):
        pltpu.make_async_copy(code.at[front], raw_in.at[front], r_in).wait()
        pltpu.make_async_copy(misc_in.at[front], misc_in.at[front], m_in).wait()


def output_kernel(slot, stat, root, raw, misc, new_out, root_out, update_out, tbuf, rscale, sems, out_sems):
    puts = [pltpu.make_async_copy(root, root_out.at[0], sems.at[0]), pltpu.make_async_copy(stat, new_out, sems.at[1])]
    for c in puts:
        c.start()
    me = lax.axis_index(AXIS)
    source = lax.broadcasted_iota(I32, (N, 1, 1), 0)
    turn = lax.rem(8 + me // 32 - source // 32 + lax.rem(me // 2, 4) - lax.rem(source // 2, 4), 4)
    lane = lax.broadcasted_iota(I32, (1, 1, 128), 2)

    def pick(v, at):
        return jnp.sum(jnp.where(lane == at, v, 0.0), axis=2, keepdims=True)

    values = misc[...]
    totals = jnp.sum(values, axis=0, keepdims=True)
    graft = jnp.sqrt(pick(totals, 8)) / jnp.sqrt(pick(totals, 9))
    rscale[...] = jnp.broadcast_to(pick(values, turn) * graft, (N, 1, 128))
    step = 16

    def chunk(i, carry):
        part = pl.ds(i * step, step)
        for j in range(step):
            b = i * step + j
            s = slot[b]
            value = rscale[s]
            for c in range(8):
                cols = slice(128 * c, 128 * (c + 1))
                tbuf[b, :, cols] = quarter_value(raw[s, :, cols], value)
        pltpu.make_async_copy(tbuf.at[part], update_out.at[part], out_sems.at[i]).start()
        return carry

    lax.fori_loop(0, N // step, chunk, 0)
    for i in range(N // step):
        part = pl.ds(i * step, step)
        pltpu.make_async_copy(tbuf.at[part], update_out.at[part], out_sems.at[i]).wait()
    for c in puts:
        c.wait()


def body(statistics, gradient, block_slot):
    in_hbm = pl.BlockSpec(memory_space=pltpu.HBM)
    smem = pl.BlockSpec(memory_space=pltpu.SMEM)
    vmem = pl.BlockSpec(memory_space=pltpu.VMEM)
    dma = pltpu.SemaphoreType.DMA
    V = pltpu.VMEM
    statistics = pltpu.with_memory_space_constraint(statistics, pltpu.HBM)
    gradient = pltpu.with_memory_space_constraint(gradient, pltpu.HBM)
    block_slot = pltpu.with_memory_space_constraint(block_slot, pltpu.HBM)
    stat, root, raw_rows, misc = pl.pallas_call(
        exchange_kernel,
        out_shape=(
            jax.ShapeDtypeStruct((N, ROWS, B), F32),
            jax.ShapeDtypeStruct((B, B), F32),
            jax.ShapeDtypeStruct((N, ROWS, B), I16),
            jax.ShapeDtypeStruct((N, 1, 128), F32),
        ),
        in_specs=[in_hbm, in_hbm, in_hbm],
        out_specs=(vmem,) * 4,
        scratch_shapes=[
            V((1, 128), I32), V((1, 128), I32), pltpu.SMEM((1, 128), I32), pltpu.SMEM((1, 128), I32),
            V((N, ROWS, B), I16),
            V((N, ROWS, B), BF16), V((N, ROWS, B), BF16), V((N, ROWS, 640), I16),
            V((N, ROWS, B), BF16), V((N, ROWS, 640), I16), V((B, B), BF16),
            V((B, B), F32), V((B, B), F32),
            V((B, B), BF16), V((B, B), F8), V((B, B), F8), V((B, B), BF16), V((B, B), BF16), V((2, B, B), BF16),
            V((N, ROWS, B), I16), V((1, 128), F32),
        ]
        + [dma] * 16,
        compiler_params=pltpu.CompilerParams(
            collective_id=0, has_side_effects=True, vmem_limit_bytes=43 * 1024 * 1024
        ),
        name="exchange",
    )(block_slot, statistics, gradient)
    return pl.pallas_call(
        output_kernel,
        out_shape=(
            jax.ShapeDtypeStruct((N, ROWS, B), F32),
            jax.ShapeDtypeStruct((1, B, B), F32),
            jax.ShapeDtypeStruct((N, ROWS, B), F32),
        ),
        in_specs=[smem, vmem, vmem, vmem, vmem],
        out_specs=(in_hbm, in_hbm, in_hbm),
        scratch_shapes=[
            V((N, ROWS, B), F32), V((N, 1, 128), F32), dma((2,)), dma((8,)),
        ],
        compiler_params=pltpu.CompilerParams(vmem_limit_bytes=16 * 1024 * 1024),
        name="outputs",
    )(block_slot, stat, root, raw_rows, misc)


def solution(mesh):
    rows = P(None, AXIS, None)
    return jax.shard_map(
        body, mesh=mesh, in_specs=(rows, rows, P()), out_specs=(rows, P(AXIS, None, None), rows), check_vma=False
    )
```
